32 devices in a mesh: cuts: 8 (over y, x, core), tr: 4 (over z).
Axes of the slice: x: 2, y: 2, z: 4, core: 2. Of those that a mesh axis runs over, the one named last changes fastest.
Arguments:
- cells: int32 [2, 8, 2, 1024], P(None, 'cuts'), may hold values from 1 to 509
- offsets: float32 [2, 8, 2, 1024], P(None, 'cuts'), may hold values from 0 to 1
- charges: float32 [2, 8, 1024], P(None, 'cuts'), may hold values from 0.5 to 2
- momenta: float32 [2, 8, 2, 1024], P(None, 'cuts', None, 'tr'), may hold values from -6 to 6
- green: float32 [1024, 1024], replicated, may hold values from -0.1875 to 0.1875
Outputs:
- momenta_out: float32 [2, 8, 2, 1024], P(None, 'cuts', None, 'tr')
The draws below stay inside these ranges and needn't reach their ends.
Inputs may be any that keep to these rules, and one draw needn't show every extreme that they name: `cells`: every cell index lies in 1 .. 509.
All inputs are finite; a program needn't handle non-finite values.
Results may differ from the reference program's by a relative error of at most 0.017.
Values may be sent and summed in bfloat16 or wider, within the bound.
No kernel may reach another device: no remote copies, remote signals or barrier semaphores. Data moves between devices by JAX's collectives and lax.ppermute only.
A program may use at most 64 MiB of HBM per device.

```python
import math
import jax
import jax.numpy as jnp
from jax import lax

G = 512
NP = 1024
SECTIONS = 4
PAD = 1024
SL = 8


def with_ends(array, own_key, least, high):
    longest = array.shape.index(max(array.shape))
    spots = []
    for shift in (0, 1):
        where = [jax.random.randint(jax.random.fold_in(own_key, axis), (), 0, length) for axis, length in enumerate(array.shape)]
        where[longest] = (where[longest] + shift) % array.shape[longest]
        spots.append(tuple(where))
    return array.at[spots[0]].set(least).at[spots[1]].set(high)


def steps_of(stream_key, dims, split, low, largest):
    factor_of, own = 1.0, jax.random.fold_in(stream_key, 6)
    for dim, blocks in split:
        draws = jnp.exp(jax.random.uniform(jax.random.fold_in(own, dim), (blocks,), jnp.float32, low / len(split), largest / len(split)))
        factor_of = factor_of * jnp.repeat(draws, dims[dim] // blocks).reshape([-1 if axis == dim else 1 for axis in range(len(dims))])
    return factor_of


def gaussian(stream_key, shape, scale, most, cuts=(), kind=jnp.bfloat16):
    result = jax.random.normal(stream_key, shape, jnp.float32) * scale
    if len(cuts) > 0:
        result = steps_of(stream_key, shape, cuts, -0.22, 0.18) * result
    return jnp.clip(result, min=-most, max=most).astype(kind)


def setup_inputs(seed: int = 0) -> dict:
    keys = jax.random.split(jax.random.key(seed), 6)
    return {
        "cells": with_ends(jax.random.randint(keys[0], (2, SL, 2, NP), 1, G - 2), jax.random.fold_in(keys[0], 1), 1, (G - 2) - 1).astype(jnp.int32),
        "offsets": jnp.clip(1.0 * jax.random.uniform(keys[1], (2, SL, 2, NP), jnp.float32) ** steps_of(keys[1], (2, SL, 2, NP), ((1, 8),), -0.2, 0.2), 0.0, 1.0),
        "charges": jnp.clip(jnp.exp(math.log(2.0) - 1.3862944 * jax.random.uniform(keys[2], (2, SL, NP), jnp.float32) ** steps_of(keys[2], (2, SL, NP), ((1, 8),), -0.2, 0.2)), 0.5, 2.0),
        "momenta": gaussian(keys[3], (2, SL, 2, NP), 1.0, 6.0, ((1, 8), (3, 4)), jnp.float32),
        "green": gaussian(keys[4], (PAD, PAD), NP ** -0.5, 0.1875, (), jnp.float32),
    }


drift_step = 0.5


def rounded(values):
    return lax.optimization_barrier(values.astype(jnp.bfloat16)).astype(jnp.float32)


def product(left, right):
    return jnp.dot(left, right, precision=lax.Precision.HIGHEST)


def phase_angles(frequency, position, period):
    return (2.0 * math.pi / period) * ((frequency * position) % period).astype(jnp.float32)


def make_tables(period):
    counter = jnp.arange(period, dtype=jnp.int32)
    theta = phase_angles(counter[:, None], counter[None, :], period)
    return rounded(jnp.cos(theta)), rounded(jnp.sin(theta))


def slice_weights(cells, offsets, charges):
    row_low = rounded(1.0 - offsets[0])
    row_high = rounded(offsets[0])
    col_low = rounded(1.0 - offsets[1])
    col_high = rounded(offsets[1])
    charge_low = rounded(charges * (1.0 - offsets[1]))
    charge_high = rounded(charges * offsets[1])
    return row_low, row_high, col_low, col_high, charge_low, charge_high


def deposit(cells, offsets, charges):
    row_low, row_high, col_low, col_high, charge_low, charge_high = slice_weights(cells, offsets, charges)
    row_cells = cells[0]
    col_cells = cells[1]
    charge_grid = jnp.zeros((G, G), jnp.float32)
    charge_grid = charge_grid.at[row_cells, col_cells].add(row_low * charge_low)
    charge_grid = charge_grid.at[row_cells, col_cells + 1].add(row_low * charge_high)
    charge_grid = charge_grid.at[row_cells + 1, col_cells].add(row_high * charge_low)
    charge_grid = charge_grid.at[row_cells + 1, col_cells + 1].add(row_high * charge_high)
    return rounded(charge_grid)


def potentials(one, two, cosine, sine, kernel_re, kernel_im):
    cos_head = cosine[:G]
    sin_head = sine[:G]
    cos_left = cosine[:, :G]
    sin_left = sine[:, :G]
    first_re = rounded(product(one, cos_head) + product(two, sin_head))
    first_im = rounded(product(two, cos_head) - product(one, sin_head))
    second_re = product(cos_left, first_re) + product(sin_left, first_im)
    second_im = product(cos_left, first_im) - product(sin_left, first_re)
    scaled_re = rounded(second_re * kernel_re - second_im * kernel_im)
    scaled_im = rounded(second_re * kernel_im + second_im * kernel_re)
    back_re = rounded(product(cos_head, scaled_re) - product(sin_head, scaled_im))
    back_im = rounded(product(cos_head, scaled_im) + product(sin_head, scaled_re))
    phi_one = (product(back_re, cos_left) - product(back_im, sin_left)) / (PAD * PAD)
    phi_two = (product(back_im, cos_left) + product(back_re, sin_left)) / (PAD * PAD)
    return phi_one, phi_two


def field_pair(potential):
    widened = jnp.pad(potential, 1)
    along_rows = (widened[:-2, 1:-1] - widened[2:, 1:-1]) * 0.5
    along_cols = (widened[1:-1, :-2] - widened[1:-1, 2:]) * 0.5
    return rounded(along_rows), rounded(along_cols)


def slice_kicks(cells, offsets, field_rows, field_cols):
    row_low, row_high, col_low, col_high, charge_low, charge_high = slice_weights(cells, offsets, offsets[0])
    row_cells = cells[0]
    col_cells = cells[1]

    def sample(field):
        total_low = col_low * field[row_cells, col_cells] + col_high * field[row_cells, col_cells + 1]
        total_high = col_low * field[row_cells + 1, col_cells] + col_high * field[row_cells + 1, col_cells + 1]
        return row_low * total_low + row_high * total_high

    return jnp.stack([sample(field_rows), sample(field_cols)])


def drift(cells, offsets, moment):
    place = cells.astype(jnp.float32) + offsets + drift_step * moment
    place = jnp.clip(place, 1.0, G - 2.0 - 1.0 / 64.0)
    whole = jnp.floor(place)
    return whole.astype(jnp.int32), place - whole


def reference(cells, offsets, charges, momenta, green):
    cosine, sine = make_tables(PAD)
    kernel_grid = rounded(green)
    kernel_cos = rounded(product(kernel_grid, cosine))
    kernel_sin = rounded(-product(kernel_grid, sine))
    kernel_re = product(cosine, kernel_cos) + product(sine, kernel_sin)
    kernel_im = product(cosine, kernel_sin) - product(sine, kernel_cos)
    moment = momenta
    for section_index in range(SECTIONS):
        grids = jax.vmap(jax.vmap(deposit))(cells, offsets, charges)
        visitors = jnp.roll(grids[1], -2 * section_index, axis=0)

        def meeting(inputs):
            phi_one, phi_two = potentials(inputs[0], inputs[1], cosine, sine, kernel_re, kernel_im)
            return field_pair(phi_one), field_pair(phi_two)

        fields_one, fields_two = lax.map(meeting, (grids[0], visitors))
        kick_one = jax.vmap(slice_kicks)(cells[0], offsets[0], fields_two[0], fields_two[1])
        moved_rows = jnp.roll(fields_one[0], 2 * section_index, axis=0)
        moved_cols = jnp.roll(fields_one[1], 2 * section_index, axis=0)
        kick_two = jax.vmap(slice_kicks)(cells[1], offsets[1], moved_rows, moved_cols)
        moment = moment + jnp.stack([kick_one, kick_two])
        if section_index + 1 < SECTIONS:
            cells, offsets = drift(cells, offsets, moment)
    return moment
```

```python
import functools
import math

import jax
import jax.numpy as jnp
import numpy as np
from jax import lax
from jax.experimental import pallas as pl
from jax.experimental.pallas import tpu as pltpu
from jax.sharding import PartitionSpec as P

SECTIONS = 4
DRIFT_STEP = 0.5
GROUP = 16
VMEM_LIMIT = 40 * 1024 * 1024

VMEM = pl.BlockSpec(memory_space=pltpu.VMEM)
ANY = pl.BlockSpec(memory_space=pl.ANY)


def dot_nn(left, right):
    return jnp.dot(left, right, preferred_element_type=jnp.float32)


def dot_nt(left, right):
    return lax.dot_general(
        left, right, (((1,), (1,)), ((), ())), preferred_element_type=jnp.float32
    )


def phases(products, period):
    theta = 2.0 * np.pi / period * (products % period)
    return np.cos(theta).astype(np.float32), np.sin(theta).astype(np.float32)


def factors(extent, period):
    half = extent // 2
    span = np.arange(extent, dtype=np.int64)
    odd = 2 * span + 1
    fine = np.arange(GROUP, dtype=np.int64)
    coarse = np.arange(extent // GROUP, dtype=np.int64)
    col_coarse = phases(2 * GROUP * coarse[:, None] * span[None, :], 2 * period)
    col_fine = phases((2 * fine + 1)[:, None] * span[None, :], 2 * period)
    inv_coarse = phases(GROUP * coarse[:, None] * odd[None, :], 2 * period)
    inv_fine = phases(fine[:, None] * odd[None, :], 2 * period)
    rows = np.arange(half, dtype=np.int64)
    row_coarse = phases(4 * GROUP * np.arange(half // GROUP)[:, None] * rows[None, :], period)
    starts = (4 * fine[None, :] + np.arange(4)[:, None]).reshape(-1)
    row_fine = phases(starts[:, None] * rows[None, :], period)
    return col_coarse + col_fine + inv_coarse + inv_fine + row_coarse + row_fine


def quarter_sums(lower, upper):
    (low_re, low_im), (high_re, high_im) = lower, upper
    return (
        (low_re + high_re, low_im + high_im),
        (low_re + high_im, low_im - high_re),
        (low_re - high_re, low_im - high_im),
        (low_re - high_im, low_im + high_re),
    )


def joined(pair):
    return jnp.concatenate([pair[0].astype(jnp.bfloat16), pair[1].astype(jnp.bfloat16)], axis=1)


def setup_kernel(
    green_ref,
    cc_cos, cc_sin, cf_cos, cf_sin,
    ic_cos, ic_sin, if_cos, if_sin,
    rc_cos, rc_sin, rf_cos, rf_sin,
    col_ref, inv_ref, row_ref, spec_ref,
    green_vm, sem,
):
    extent = cc_cos.shape[1]
    half = extent // 2
    period = green_ref.shape[0]
    copies = [
        pltpu.make_async_copy(
            green_ref.at[pl.ds(q * half, half)], green_vm.at[pl.ds(q * half, half)], sem.at[q]
        )
        for q in range(4)
    ]
    for copy in copies:
        copy.start()

    for i in range(extent // GROUP):
        rows = slice(i * GROUP, (i + 1) * GROUP)
        lower = slice(extent + i * GROUP, extent + (i + 1) * GROUP)
        ca, sa = cc_cos[i : i + 1, :], cc_sin[i : i + 1, :]
        cb, sb = cf_cos[...], cf_sin[...]
        col_ref[rows, :] = (ca * cb - sa * sb).astype(jnp.bfloat16)
        col_ref[lower, :] = (-(sa * cb + ca * sb)).astype(jnp.bfloat16)
        ca, sa = ic_cos[i : i + 1, :], ic_sin[i : i + 1, :]
        cb, sb = if_cos[...], if_sin[...]
        inv_ref[rows, :extent] = (ca * cb - sa * sb).astype(jnp.bfloat16)
        inv_ref[rows, extent:] = (-(sa * cb + ca * sb)).astype(jnp.bfloat16)
    for j in range(4):
        cb, sb = rf_cos[j * GROUP : (j + 1) * GROUP, :], rf_sin[j * GROUP : (j + 1) * GROUP, :]
        for i in range(half // GROUP):
            upper = slice(i * GROUP, (i + 1) * GROUP)
            lower = slice(half + i * GROUP, half + (i + 1) * GROUP)
            ca, sa = rc_cos[i : i + 1, :], rc_sin[i : i + 1, :]
            cosine = (ca * cb - sa * sb).astype(jnp.bfloat16)
            sine = sa * cb + ca * sb
            minus = (-sine).astype(jnp.bfloat16)
            sine = sine.astype(jnp.bfloat16)
            row_ref[j, upper, :half] = cosine
            row_ref[j, upper, half:] = sine
            row_ref[j, lower, :half] = minus
            row_ref[j, lower, half:] = cosine

    for copy in copies:
        copy.wait()
    scale = 1.0 / (period * period)
    chunk = math.gcd(extent, 256)
    for begin in range(0, extent, chunk):
        parity = lax.broadcasted_iota(jnp.int32, (chunk, half), 0) + begin
        sign = jnp.where(parity % 2 == 0, 1.0, -1.0)
        table = jnp.concatenate(
            [col_ref[begin : begin + chunk, :], col_ref[extent + begin : extent + begin + chunk, :]],
            axis=0,
        )
        parts = []
        for q in range(4):
            block = green_vm[q * half : (q + 1) * half, :].astype(jnp.bfloat16)
            near = dot_nt(table, block[:, :extent])
            far = dot_nt(table, block[:, extent:])
            parts.append(
                (near[:chunk] - sign * far[chunk:], near[chunk:] + sign * far[:chunk])
            )
        (a, b, c, d) = parts
        even = (a[0] + c[0], a[1] + c[1])
        even_less = (a[0] - c[0], a[1] - c[1])
        odd = (b[0] + d[0], b[1] + d[1])
        odd_less = (b[0] - d[0], b[1] - d[1])
        sums = (
            (even[0] + odd[0], even[1] + odd[1]),
            (even_less[0] + odd_less[1], even_less[1] - odd_less[0]),
            (even[0] - odd[0], even[1] - odd[1]),
            (even_less[0] - odd_less[1], even_less[1] + odd_less[0]),
        )
        for j in range(4):
            spec_ref[j, begin : begin + chunk, :] = dot_nt(joined(sums[j]), row_ref[j]) * scale


def hat_rows(position, count):
    nodes = lax.broadcasted_iota(jnp.int32, (count, position.shape[1]), 0).astype(jnp.float32)
    return jnp.maximum(1.0 - jnp.abs(nodes - position), 0.0)


def kicks(guest_rows, guest_cols, guest_charge, rows, cols, col_ref, inv_ref, row_ref, spec_ref, back_ref):
    extent = col_ref.shape[1]
    half = extent // 2
    weight_rows = hat_rows(guest_rows, extent).astype(jnp.bfloat16)
    weight_cols = (guest_charge * hat_rows(guest_cols, extent)).astype(jnp.bfloat16)
    grid = dot_nt(weight_cols, weight_rows).astype(jnp.bfloat16)
    chunk = math.gcd(extent, 256)
    for begin in range(0, extent, chunk):
        here = slice(begin, begin + chunk)
        there = slice(extent + begin, extent + begin + chunk)
        real = dot_nn(col_ref[here, :], grid)
        imag = dot_nn(col_ref[there, :], grid)
        sums = quarter_sums(
            (real[:, :half], imag[:, :half]), (real[:, half:], imag[:, half:])
        )
        backs = []
        for j in range(4):
            forward = dot_nt(joined(sums[j]), row_ref[j])
            kernel_re = spec_ref[j, here, :half]
            kernel_im = spec_ref[j, here, half:]
            forward_re, forward_im = forward[:, :half], forward[:, half:]
            scaled = joined(
                (
                    forward_re * kernel_re - forward_im * kernel_im,
                    forward_re * kernel_im + forward_im * kernel_re,
                )
            )
            back = dot_nn(scaled, row_ref[j])
            backs.append((back[:, :half], back[:, half:]))
        (a, b, c, d) = backs
        even = (a[0] + c[0], a[1] + c[1])
        even_less = (a[0] - c[0], a[1] - c[1])
        odd = (b[0] + d[0], b[1] + d[1])
        odd_less = (b[0] - d[0], b[1] - d[1])
        back_ref[here, :] = joined((even[0] + odd[0], even_less[0] - odd_less[1]))
        back_ref[there, :] = joined((even[1] + odd[1], even_less[1] + odd_less[0]))
    potential = dot_nn(inv_ref[...], back_ref[...])
    zero_lane = jnp.zeros((extent, 1), jnp.float32)
    zero_row = jnp.zeros((1, extent), jnp.float32)
    before = jnp.concatenate([zero_lane, potential[:, :-1]], axis=1)
    after = jnp.concatenate([potential[:, 1:], zero_lane], axis=1)
    along_rows = (before - after).astype(jnp.bfloat16)
    before = jnp.concatenate([zero_row, potential[:-1, :]], axis=0)
    after = jnp.concatenate([potential[1:, :], zero_row], axis=0)
    along_cols = (before - after).astype(jnp.bfloat16)
    weight_rows = hat_rows(rows, extent).astype(jnp.bfloat16)
    weight_cols = hat_rows(cols, extent).astype(jnp.bfloat16).astype(jnp.float32)
    kick_rows = jnp.sum(dot_nn(along_rows, weight_rows) * weight_cols, axis=0, keepdims=True)
    kick_cols = jnp.sum(dot_nn(along_cols, weight_rows) * weight_cols, axis=0, keepdims=True)
    return kick_rows, kick_cols


def advance(position, moment, extent):
    return jnp.clip(position + DRIFT_STEP * moment, 1.0, extent - 2.0 - 1.0 / 64.0)


def section_kernel(last, guest_ref, own_ref, moment_ref, col_ref, inv_ref, row_ref, spec_ref, *rest):
    extent = col_ref.shape[1]
    back_ref = rest[-1]
    rows, cols = own_ref[0:1, :], own_ref[1:2, :]
    kick_rows, kick_cols = kicks(
        guest_ref[0:1, :], guest_ref[1:2, :], guest_ref[2:3, :], rows, cols,
        col_ref, inv_ref, row_ref, spec_ref, back_ref,
    )
    moment_rows = moment_ref[0:1, :] + kick_rows
    moment_cols = moment_ref[1:2, :] + kick_cols
    out_moment_ref = rest[0]
    out_moment_ref[0:1, :] = moment_rows
    out_moment_ref[1:2, :] = moment_cols
    if not last:
        out_ref = rest[1]
        out_ref[0:1, :] = advance(rows, moment_rows, extent)
        out_ref[1:2, :] = advance(cols, moment_cols, extent)
        out_ref[2:4, :] = own_ref[2:4, :]


def per_device(cells, offsets, charges, momenta, green):
    shards = lax.axis_size("tr")
    slices = lax.axis_size("cuts")
    shard = lax.axis_index("tr")
    period = green.shape[0]
    extent = period // 2
    half = extent // 2
    particles = cells.shape[-1]
    own_count = momenta.shape[-1]
    role = shard % 2

    def slot(cut, part):
        return (cut % slices) * shards + part

    def exchange(value, steps):
        pairs = []
        for cut in range(slices):
            for part in range(shards):
                turn = steps if part % 2 == 1 else -steps
                pairs.append((slot(cut, part), slot(cut + turn, part ^ 1)))
        return lax.ppermute(value, ("cuts", "tr"), pairs)

    pieces = [lax.dynamic_index_in_dim(momenta[:, 0], 1 - role, 0, keepdims=False)]
    for step in range(1, shards):
        wanted = 1 - (shard + step) % 2
        sent = lax.dynamic_index_in_dim(momenta[:, 0], wanted, 0, keepdims=False)
        pieces.append(
            lax.ppermute(sent, "tr", [(i, (i + step) % shards) for i in range(shards)])
        )
    moment = jnp.concatenate(pieces[::-1], axis=1)
    moment = jnp.roll(moment, (shard + 1) * own_count, axis=1)

    position = cells[:, 0].astype(jnp.float32) + offsets[:, 0]
    packets = jnp.concatenate(
        [position, charges[:, 0][:, None], jnp.zeros((2, 1, particles), jnp.float32)], axis=1
    )
    own = lax.dynamic_index_in_dim(packets, 1 - role, 0, keepdims=False)
    guest = lax.dynamic_index_in_dim(packets, role, 0, keepdims=False)

    tables = pl.pallas_call(
        setup_kernel,
        out_shape=(
            jax.ShapeDtypeStruct((2 * extent, extent), jnp.bfloat16),
            jax.ShapeDtypeStruct((extent, 2 * extent), jnp.bfloat16),
            jax.ShapeDtypeStruct((4, extent, extent), jnp.bfloat16),
            jax.ShapeDtypeStruct((4, extent, extent), jnp.float32),
        ),
        in_specs=[ANY] + [VMEM] * 12,
        out_specs=(VMEM,) * 4,
        scratch_shapes=[
            pltpu.VMEM((period, period), jnp.float32),
            pltpu.SemaphoreType.DMA((4,)),
        ],
        compiler_params=pltpu.CompilerParams(vmem_limit_bytes=VMEM_LIMIT),
        cost_estimate=pl.CostEstimate(
            flops=3 * period**3, bytes_accessed=8 * period**2, transcendentals=0
        ),
        name="setup",
    )(green, *[jnp.asarray(value) for value in factors(extent, period)])

    for section in range(SECTIONS):
        last = section + 1 == SECTIONS
        if section > 0:
            guest = exchange(own, 2 * section)
        shapes = [jax.ShapeDtypeStruct((2, particles), jnp.float32)]
        if not last:
            shapes.append(jax.ShapeDtypeStruct((4, particles), jnp.float32))
        results = pl.pallas_call(
            functools.partial(section_kernel, last),
            out_shape=tuple(shapes),
            in_specs=[VMEM] * 7,
            out_specs=(VMEM,) * len(shapes),
            scratch_shapes=[pltpu.VMEM((2 * extent, extent), jnp.bfloat16)],
            compiler_params=pltpu.CompilerParams(vmem_limit_bytes=VMEM_LIMIT),
            cost_estimate=pl.CostEstimate(
                flops=5 * period**3, bytes_accessed=8 * period**2, transcendentals=0
            ),
            name="section",
        )(guest, own, moment, *tables)
        moment = results[0]
        if not last:
            own = results[1]

    mine = lax.dynamic_slice_in_dim(moment, shard * own_count, own_count, axis=1)
    partner = shard + 1 - 2 * role
    theirs = lax.dynamic_slice_in_dim(moment, partner * own_count, own_count, axis=1)
    received = exchange(theirs, 0)
    first = jnp.where(role == 1, mine, received)
    second = jnp.where(role == 1, received, mine)
    return jnp.stack([first, second])[:, None]


def solution(mesh):
    return jax.shard_map(
        per_device,
        mesh=mesh,
        in_specs=(
            P(None, "cuts", None, None),
            P(None, "cuts", None, None),
            P(None, "cuts", None),
            P(None, "cuts", None, "tr"),
            P(),
        ),
        out_specs=P(None, "cuts", None, "tr"),
        check_vma=False,
    )
```

```python
import functools
import math

import jax
import jax.numpy as jnp
import numpy as np
from jax import lax
from jax.experimental import pallas as pl
from jax.experimental.pallas import tpu as pltpu
from jax.sharding import PartitionSpec as P

SECTIONS = 4
DRIFT_STEP = 0.5
GROUP = 16
SETUP_VMEM = 54 * 1024 * 1024
SECTION_VMEM = 28 * 1024 * 1024
HALF_ROOT = math.sqrt(0.5)

VMEM = pl.BlockSpec(memory_space=pltpu.VMEM)
HBM = pl.BlockSpec(memory_space=pltpu.MemorySpace.HBM)


def dot_nn(left, right):
    return jnp.dot(left, right, preferred_element_type=jnp.float32)


def dot_nt(left, right):
    return lax.dot_general(
        left, right, (((1,), (1,)), ((), ())), preferred_element_type=jnp.float32
    )


def phases(products, period):
    theta = 2.0 * np.pi / period * (products % period)
    return np.cos(theta).astype(np.float32), np.sin(theta).astype(np.float32)


def factors(extent):
    half = extent // 2
    eighth = extent // 4
    period = 2 * extent
    cells = np.arange(extent, dtype=np.int64)
    split = np.concatenate([cells[0::2], cells[1::2]])
    odd = 2 * cells[:half] + 1
    fine = np.arange(GROUP, dtype=np.int64)
    coarse = np.arange(half // GROUP, dtype=np.int64)
    few = np.arange(eighth // GROUP, dtype=np.int64)
    starts = (8 * fine[None, :] + np.arange(8)[:, None]).reshape(-1)
    pieces = []
    for order in (split, cells):
        pieces += phases(2 * GROUP * coarse[:, None] * order[None, :], 2 * period)
        pieces += phases((2 * fine + 1)[:, None] * order[None, :], 2 * period)
    for rows in (2 * GROUP * coarse, 2 * fine, 2 * fine + 1):
        pieces.append(np.concatenate(phases(rows[:, None] * odd[None, :], 2 * period), axis=1))
    for rows in (8 * GROUP * few, starts):
        both = np.concatenate(phases(rows[:, None] * cells[None, :eighth], period), axis=1)
        pieces.append(np.concatenate([both, both], axis=1))
    begins = np.cumsum([0] + [piece.shape[0] for piece in pieces])
    total = -(-int(begins[-1]) // 8) * 8
    packed = np.zeros((total, extent), np.float32)
    packed[: begins[-1]] = np.concatenate(pieces, axis=0)
    return packed, [int(begin) for begin in begins[:-1]]


def turned(cos_a, sin_a, cos_b, sin_b):
    return cos_a * cos_b - sin_a * sin_b, sin_a * cos_b + cos_a * sin_b


def added(left, right):
    return left[0] + right[0], left[1] + right[1]


def less(left, right):
    return left[0] - right[0], left[1] - right[1]


def times_i(value):
    return -value[1], value[0]


def four_points(values, turn):
    even, even_less = added(values[0], values[2]), less(values[0], values[2])
    odd, odd_less = added(values[1], values[3]), less(values[1], values[3])
    side = times_i(odd_less)
    up, down = added(even_less, side), less(even_less, side)
    if turn < 0:
        up, down = down, up
    return added(even, odd), up, less(even, odd), down


def eighths(values, turn):
    first, second, third, fourth = values
    plus = ((second[0] - turn * second[1]) * HALF_ROOT, (second[1] + turn * second[0]) * HALF_ROOT)
    third = times_i(third)
    if turn < 0:
        third = (-third[0], -third[1])
    minus = (
        (-fourth[0] - turn * fourth[1]) * HALF_ROOT,
        (turn * fourth[0] - fourth[1]) * HALF_ROOT,
    )
    return first, plus, third, minus


def joined(pair):
    return jnp.concatenate([pair[0].astype(jnp.bfloat16), pair[1].astype(jnp.bfloat16)], axis=1)


def spread(values):
    even = four_points(values, -1)
    odd = four_points(eighths(values, -1), -1)
    return [pair for couple in zip(even, odd) for pair in couple]


def gathered(values):
    even = four_points(values[0::2], 1)
    odd = eighths(four_points(values[1::2], 1), 1)
    return [added(left, right) for left, right in zip(even, odd)]


def setup_kernel(begins, green_ref, factor_ref, col_ref, inv_ref, row_ref, spec_ref,
                 wide_ref, green_vm, factor_vm, sem):
    extent = col_ref.shape[1]
    half = extent // 2
    eighth = extent // 4
    period = 2 * extent
    first = pltpu.make_async_copy(factor_ref, factor_vm, sem.at[8])
    first.start()
    copies = [
        pltpu.make_async_copy(
            green_ref.at[pl.ds(q * eighth, eighth)], green_vm.at[pl.ds(q * eighth, eighth)], sem.at[q]
        )
        for q in range(8)
    ]
    for copy in copies:
        copy.start()
    first.wait()

    def column_tables(base, i):
        cos_a = factor_vm[begins[base] + i : begins[base] + i + 1, :]
        sin_a = factor_vm[begins[base + 1] + i : begins[base + 1] + i + 1, :]
        cos_b = factor_vm[begins[base + 2] : begins[base + 2] + GROUP, :]
        sin_b = factor_vm[begins[base + 3] : begins[base + 3] + GROUP, :]
        return turned(cos_a, sin_a, cos_b, sin_b)

    parity = lax.broadcasted_iota(jnp.int32, (GROUP, extent), 1) % 2
    flip = jnp.where(parity == 0, 1.0, -1.0)
    for i in range(half // GROUP):
        rows = i * GROUP
        cosine, sine = column_tables(0, i)
        col_ref[rows : rows + GROUP, :] = cosine.astype(jnp.bfloat16)
        col_ref[half + rows : half + rows + GROUP, :] = (-sine).astype(jnp.bfloat16)
        cosine, sine = column_tables(4, i)
        block = rows // eighth * extent + rows % eighth
        for turn in range(2):
            if turn:
                cosine, sine = cosine * flip, sine * flip
            at = block + turn * eighth
            wide_ref[at : at + GROUP, :] = cosine.astype(jnp.bfloat16)
            wide_ref[at + half : at + half + GROUP, :] = (-sine).astype(jnp.bfloat16)
        coarse = factor_vm[begins[8] + i : begins[8] + i + 1, :]
        for turn in range(2):
            fine = factor_vm[begins[9 + turn] : begins[9 + turn] + GROUP, :]
            cosine, sine = turned(coarse[:, :half], coarse[:, half:], fine[:, :half], fine[:, half:])
            at = turn * half + rows
            inv_ref[at : at + GROUP, :half] = cosine.astype(jnp.bfloat16)
            inv_ref[at : at + GROUP, half:] = (-sine).astype(jnp.bfloat16)
    for j in range(8):
        fine = factor_vm[begins[12] + j * GROUP : begins[12] + (j + 1) * GROUP, :]
        for i in range(eighth // GROUP):
            coarse = factor_vm[begins[11] + i : begins[11] + i + 1, :]
            cosine, sine = turned(
                coarse[:, :eighth], coarse[:, eighth:half], fine[:, :eighth], fine[:, eighth:half]
            )
            upper = i * GROUP
            lower = eighth + i * GROUP
            row_ref[j, upper : upper + GROUP, :eighth] = cosine.astype(jnp.bfloat16)
            row_ref[j, upper : upper + GROUP, eighth:] = sine.astype(jnp.bfloat16)
            row_ref[j, lower : lower + GROUP, :eighth] = (-sine).astype(jnp.bfloat16)
            row_ref[j, lower : lower + GROUP, eighth:] = cosine.astype(jnp.bfloat16)

    for copy in copies:
        copy.wait()
    scale = 1.0 / (period * period)
    parity = lax.broadcasted_iota(jnp.int32, (half, eighth), 0) % 2
    sign = jnp.where(parity == 0, 1.0, -1.0)
    for begin in range(0, extent, half):
        table = wide_ref[2 * begin : 2 * begin + extent, :]
        parts = []
        for q in range(8):
            block = green_vm[q * eighth : (q + 1) * eighth, :].astype(jnp.bfloat16)
            near = dot_nt(table, block[:, :extent])
            far = dot_nt(table, block[:, extent:])
            parts.append((near[:half] - sign * far[half:], near[half:] + sign * far[:half]))
        even = four_points([added(parts[q], parts[q + 4]) for q in range(4)], -1)
        odd = four_points(eighths([less(parts[q], parts[q + 4]) for q in range(4)], -1), -1)
        sums = [pair for couple in zip(even, odd) for pair in couple]
        for j in range(8):
            spec_ref[j, begin : begin + half, :] = dot_nt(joined(sums[j]), row_ref[j]) * scale


def hats(nodes, position):
    return jnp.maximum(1.0 - jnp.abs(nodes - position), 0.0)


def row_hats(position, extent):
    nodes = lax.broadcasted_iota(jnp.int32, (extent, position.shape[1]), 0)
    return hats(nodes.astype(jnp.float32), position)


def column_hats(position, extent):
    nodes = 2 * lax.broadcasted_iota(jnp.int32, (extent // 2, position.shape[1]), 0)
    nodes = nodes.astype(jnp.float32)
    return jnp.concatenate([hats(nodes, position), hats(nodes + 1.0, position)], axis=0)


def kicks(guest_rows, guest_cols, guest_charge, rows, cols, col_ref, inv_ref, row_ref, spec_ref, back_ref):
    extent = col_ref.shape[1]
    half = extent // 2
    eighth = extent // 4
    weight_rows = row_hats(guest_rows, extent).astype(jnp.bfloat16)
    weight_cols = (guest_charge * column_hats(guest_cols, extent)).astype(jnp.bfloat16)
    grid = dot_nt(weight_cols, weight_rows).astype(jnp.bfloat16)
    for turn in range(2):
        at = turn * eighth
        re_rows = slice(at, at + eighth)
        im_rows = slice(half + at, half + at + eighth)
        table = jnp.concatenate([col_ref[re_rows, :], col_ref[im_rows, :]], axis=0)
        even = dot_nn(table[:, :half], grid[:half])
        odd = dot_nn(table[:, half:], grid[half:])
        plus, minus = even + odd, even - odd
        real = jnp.concatenate([plus[:eighth], minus[:eighth]], axis=0)
        imag = jnp.concatenate([plus[eighth:], minus[eighth:]], axis=0)
        blocks = [
            (real[:, q * eighth : (q + 1) * eighth], imag[:, q * eighth : (q + 1) * eighth])
            for q in range(4)
        ]
        here = slice(turn * half, (turn + 1) * half)
        backs = []
        for j, pair in enumerate(spread(blocks)):
            forward = dot_nt(joined(pair), row_ref[j])
            kernel_re = spec_ref[j, here, :eighth]
            kernel_im = spec_ref[j, here, eighth:]
            forward_re, forward_im = forward[:, :eighth], forward[:, eighth:]
            scaled = joined(
                (
                    forward_re * kernel_re - forward_im * kernel_im,
                    forward_re * kernel_im + forward_im * kernel_re,
                )
            )
            back = dot_nn(scaled, row_ref[j])
            backs.append((back[:, :eighth], back[:, eighth:]))
        for q, pair in enumerate(gathered(backs)):
            lanes = slice(q * eighth, (q + 1) * eighth)
            for value, where in zip(pair, (re_rows, im_rows)):
                low, high = value[:eighth], value[eighth:]
                back_ref[0, where, lanes] = (low + high).astype(jnp.bfloat16)
                back_ref[1, where, lanes] = (low - high).astype(jnp.bfloat16)
    even = dot_nn(inv_ref[:half, :], back_ref[0])
    odd = dot_nn(inv_ref[half:, :], back_ref[1])
    zero_lane = jnp.zeros((extent, 1), jnp.float32)
    zero_row = jnp.zeros((1, extent), jnp.float32)
    potential = jnp.concatenate([even, odd], axis=0)
    before = jnp.concatenate([zero_lane, potential[:, :-1]], axis=1)
    after = jnp.concatenate([potential[:, 1:], zero_lane], axis=1)
    along_rows = (before - after).astype(jnp.bfloat16)
    before = jnp.concatenate([zero_row, odd[:-1]], axis=0)
    after = jnp.concatenate([even[1:], zero_row], axis=0)
    along_cols = jnp.concatenate([before - odd, even - after], axis=0).astype(jnp.bfloat16)
    weight_rows = row_hats(rows, extent).astype(jnp.bfloat16)
    weight_cols = column_hats(cols, extent).astype(jnp.bfloat16).astype(jnp.float32)
    kick_rows = jnp.sum(dot_nn(along_rows, weight_rows) * weight_cols, axis=0, keepdims=True)
    kick_cols = jnp.sum(dot_nn(along_cols, weight_rows) * weight_cols, axis=0, keepdims=True)
    return kick_rows, kick_cols


def advance(position, moment, extent):
    return jnp.clip(position + DRIFT_STEP * moment, 1.0, extent - 2.0 - 1.0 / 64.0)


def store_moved(out_ref, moment_out_ref, rows, cols, charge, kick_rows, kick_cols, moment_rows, moment_cols, extent):
    moment_rows = moment_rows + kick_rows
    moment_cols = moment_cols + kick_cols
    moment_out_ref[0:1, :] = moment_rows
    moment_out_ref[1:2, :] = moment_cols
    out_ref[0:1, :] = advance(rows, moment_rows, extent)
    out_ref[1:2, :] = advance(cols, moment_cols, extent)
    out_ref[2:3, :] = charge
    out_ref[3:4, :] = charge


def first_kernel(shards, cells_ref, offsets_ref, charges_ref, momenta_ref, *rest):
    received = rest[:-8]
    col_ref, inv_ref, row_ref, spec_ref, out_ref, moment_out_ref, moment_ref, back_ref = rest[-8:]
    extent = col_ref.shape[1]
    shard = lax.axis_index("tr")
    role = lax.rem(shard, 2)
    own, guest = 1 - role, role
    count = momenta_ref.shape[-1]
    if count == moment_ref.shape[-1]:
        moment_ref[...] = momenta_ref[own]
    else:
        for step, piece in enumerate((momenta_ref, *received)):
            source = lax.rem(shard + shards - step, shards)
            begin = pl.multiple_of(source * count, count)
            moment_ref[:, pl.ds(begin, count)] = piece[own]
    own_place = cells_ref[own].astype(jnp.float32) + offsets_ref[own]
    guest_place = cells_ref[guest].astype(jnp.float32) + offsets_ref[guest]
    rows, cols = own_place[0:1], own_place[1:2]
    kick_rows, kick_cols = kicks(
        guest_place[0:1], guest_place[1:2], charges_ref[guest], rows, cols,
        col_ref, inv_ref, row_ref, spec_ref, back_ref,
    )
    store_moved(
        out_ref, moment_out_ref, rows, cols, charges_ref[own], kick_rows, kick_cols,
        moment_ref[0:1, :], moment_ref[1:2, :], extent,
    )


def middle_kernel(guest_ref, own_ref, moment_ref, col_ref, inv_ref, row_ref, spec_ref,
                  out_ref, moment_out_ref, back_ref):
    extent = col_ref.shape[1]
    rows, cols = own_ref[0:1, :], own_ref[1:2, :]
    kick_rows, kick_cols = kicks(
        guest_ref[0:1, :], guest_ref[1:2, :], guest_ref[2:3, :], rows, cols,
        col_ref, inv_ref, row_ref, spec_ref, back_ref,
    )
    store_moved(
        out_ref, moment_out_ref, rows, cols, own_ref[2:3, :], kick_rows, kick_cols,
        moment_ref[0:1, :], moment_ref[1:2, :], extent,
    )


def last_kernel(guest_ref, own_ref, moment_ref, col_ref, inv_ref, row_ref, spec_ref,
                mine_ref, theirs_ref, total_ref, back_ref):
    count = mine_ref.shape[1]
    kick_rows, kick_cols = kicks(
        guest_ref[0:1, :], guest_ref[1:2, :], guest_ref[2:3, :], own_ref[0:1, :], own_ref[1:2, :],
        col_ref, inv_ref, row_ref, spec_ref, back_ref,
    )
    total_ref[0:1, :] = moment_ref[0:1, :] + kick_rows
    total_ref[1:2, :] = moment_ref[1:2, :] + kick_cols
    if count == total_ref.shape[1]:
        mine_ref[...] = total_ref[...]
        theirs_ref[...] = total_ref[...]
        return
    shard = lax.axis_index("tr")
    partner = shard + 1 - 2 * lax.rem(shard, 2)
    mine_ref[...] = total_ref[:, pl.ds(pl.multiple_of(shard * count, count), count)]
    theirs_ref[...] = total_ref[:, pl.ds(pl.multiple_of(partner * count, count), count)]


def per_device(cells, offsets, charges, momenta, green):
    shards = lax.axis_size("tr")
    slices = lax.axis_size("cuts")
    period = green.shape[0]
    extent = period // 2
    particles = cells.shape[-1]
    own_count = momenta.shape[-1]

    def slot(cut, part):
        return (cut % slices) * shards + part

    def exchange(value, steps):
        pairs = []
        for cut in range(slices):
            for part in range(shards):
                turn = steps if part % 2 == 1 else -steps
                pairs.append((slot(cut, part), slot(cut + turn, part ^ 1)))
        return lax.ppermute(value, ("cuts", "tr"), pairs)

    momenta = momenta[:, 0]
    received = [
        lax.ppermute(momenta, "tr", [(i, (i + step) % shards) for i in range(shards)])
        for step in range(1, shards)
    ]
    aligned = own_count % 128 == 0
    shard = lax.axis_index("tr")
    if not aligned:
        momenta = jnp.concatenate([*received[::-1], momenta], axis=2)
        momenta = jnp.roll(momenta, (shard + 1) * own_count, axis=2)
        received = []

    packed, begins = factors(extent)
    tables = pl.pallas_call(
        functools.partial(setup_kernel, begins),
        out_shape=(
            jax.ShapeDtypeStruct((extent, extent), jnp.bfloat16),
            jax.ShapeDtypeStruct((extent, extent), jnp.bfloat16),
            jax.ShapeDtypeStruct((8, extent // 2, extent // 2), jnp.bfloat16),
            jax.ShapeDtypeStruct((8, extent, extent // 2), jnp.float32),
        ),
        in_specs=[HBM, HBM],
        out_specs=(VMEM,) * 4,
        scratch_shapes=[
            pltpu.VMEM((period, extent), jnp.bfloat16),
            pltpu.VMEM((period, period), jnp.float32),
            pltpu.VMEM(packed.shape, jnp.float32),
            pltpu.SemaphoreType.DMA((9,)),
        ],
        compiler_params=pltpu.CompilerParams(vmem_limit_bytes=SETUP_VMEM),
        cost_estimate=pl.CostEstimate(
            flops=3 * period**3, bytes_accessed=8 * period**2, transcendentals=0
        ),
        name="setup",
    )(green, jnp.asarray(packed))

    place = jax.ShapeDtypeStruct((4, particles), jnp.float32)
    moments = jax.ShapeDtypeStruct((2, particles), jnp.float32)
    piece = jax.ShapeDtypeStruct((2, own_count), jnp.float32)
    back = pltpu.VMEM((2, extent, extent), jnp.bfloat16)
    whole = pltpu.VMEM((2, particles), jnp.float32)

    def section(kernel, name, outs, scratch, arguments):
        return pl.pallas_call(
            kernel,
            out_shape=outs,
            in_specs=[VMEM] * (len(arguments) + 4),
            out_specs=(VMEM,) * len(outs),
            scratch_shapes=scratch,
            compiler_params=pltpu.CompilerParams(vmem_limit_bytes=SECTION_VMEM),
            cost_estimate=pl.CostEstimate(
                flops=3 * period**3, bytes_accessed=8 * period**2, transcendentals=0
            ),
            name=name,
        )(*arguments, *tables)

    own, moment = section(
        functools.partial(first_kernel, shards), "first", (place, moments), [whole, back],
        (cells[:, 0], offsets[:, 0], charges, momenta, *received),
    )
    for number in range(1, SECTIONS - 1):
        guest = exchange(own, 2 * number)
        own, moment = section(middle_kernel, "middle", (place, moments), [back], (guest, own, moment))
    guest = exchange(own, 2 * (SECTIONS - 1))
    role = shard % 2
    outs = (piece, piece) if aligned else (moments, moments)
    mine, theirs = section(last_kernel, "last", outs, [whole, back], (guest, own, moment))
    if not aligned:
        theirs = lax.dynamic_slice_in_dim(mine, (shard + 1 - 2 * role) * own_count, own_count, axis=1)
        mine = lax.dynamic_slice_in_dim(mine, shard * own_count, own_count, axis=1)
    received = exchange(theirs, 0)
    first = jnp.where(role == 1, mine, received)
    second = jnp.where(role == 1, received, mine)
    return jnp.stack([first, second])[:, None]


def solution(mesh):
    return jax.shard_map(
        per_device,
        mesh=mesh,
        in_specs=(
            P(None, "cuts", None, None),
            P(None, "cuts", None, None),
            P(None, "cuts", None),
            P(None, "cuts", None, "tr"),
            P(),
        ),
        out_specs=P(None, "cuts", None, "tr"),
        check_vma=False,
    )
```

```python
import functools
import math

import jax
import jax.numpy as jnp
import numpy as np
from jax import lax
from jax.experimental import pallas as pl
from jax.experimental.pallas import tpu as pltpu
from jax.sharding import PartitionSpec as P

SECTIONS = 4
DRIFT_STEP = 0.5
GROUP = 16
SETUP_VMEM = 50 * 1024 * 1024
SECTION_VMEM = 28 * 1024 * 1024
HALF_ROOT = math.sqrt(0.5)

VMEM = pl.BlockSpec(memory_space=pltpu.VMEM)
HBM = pl.BlockSpec(memory_space=pltpu.MemorySpace.HBM)


def dot_nn(left, right):
    return jnp.dot(left, right, preferred_element_type=jnp.float32)


def dot_nt(left, right):
    return lax.dot_general(
        left, right, (((1,), (1,)), ((), ())), preferred_element_type=jnp.float32
    )


def phases(products, period):
    theta = 2.0 * np.pi / period * (products % period)
    return np.cos(theta).astype(np.float32), np.sin(theta).astype(np.float32)


def factors(extent):
    half = extent // 2
    eighth = extent // 4
    period = 2 * extent
    cells = np.arange(extent, dtype=np.int64)
    split = np.concatenate([cells[0::2], cells[1::2]])
    odd = 2 * cells[:half] + 1
    fine = np.arange(GROUP, dtype=np.int64)
    coarse = np.arange(half // GROUP, dtype=np.int64)
    few = np.arange(eighth // GROUP, dtype=np.int64)
    starts = (8 * fine[None, :] + np.arange(8)[:, None]).reshape(-1)
    pieces = []
    for order in (split, cells):
        pieces += phases(2 * GROUP * coarse[:, None] * order[None, :], 2 * period)
        pieces += phases((2 * fine + 1)[:, None] * order[None, :], 2 * period)
    for rows in (2 * GROUP * coarse, 2 * fine, 2 * fine + 1):
        pieces.append(np.concatenate(phases(rows[:, None] * odd[None, :], 2 * period), axis=1))
    for rows in (8 * GROUP * few, starts):
        both = np.concatenate(phases(rows[:, None] * cells[None, :eighth], period), axis=1)
        pieces.append(np.concatenate([both, both], axis=1))
    begins = np.cumsum([0] + [piece.shape[0] for piece in pieces])
    total = -(-int(begins[-1]) // 8) * 8
    packed = np.zeros((total, extent), np.float32)
    packed[: begins[-1]] = np.concatenate(pieces, axis=0)
    return packed, [int(begin) for begin in begins[:-1]]


def turned(cos_a, sin_a, cos_b, sin_b):
    return cos_a * cos_b - sin_a * sin_b, sin_a * cos_b + cos_a * sin_b


def added(left, right):
    return left[0] + right[0], left[1] + right[1]


def less(left, right):
    return left[0] - right[0], left[1] - right[1]


def times_i(value):
    return -value[1], value[0]


def four_points(values, turn):
    even, even_less = added(values[0], values[2]), less(values[0], values[2])
    odd, odd_less = added(values[1], values[3]), less(values[1], values[3])
    side = times_i(odd_less)
    up, down = added(even_less, side), less(even_less, side)
    if turn < 0:
        up, down = down, up
    return added(even, odd), up, less(even, odd), down


def eighths(values, turn):
    first, second, third, fourth = values
    plus = ((second[0] - turn * second[1]) * HALF_ROOT, (second[1] + turn * second[0]) * HALF_ROOT)
    third = times_i(third)
    if turn < 0:
        third = (-third[0], -third[1])
    minus = (
        (-fourth[0] - turn * fourth[1]) * HALF_ROOT,
        (turn * fourth[0] - fourth[1]) * HALF_ROOT,
    )
    return first, plus, third, minus


def joined(pair):
    return jnp.concatenate([pair[0].astype(jnp.bfloat16), pair[1].astype(jnp.bfloat16)], axis=1)


def spread(values):
    even = four_points(values, -1)
    odd = four_points(eighths(values, -1), -1)
    return [pair for couple in zip(even, odd) for pair in couple]


def gathered(values):
    even = four_points(values[0::2], 1)
    odd = eighths(four_points(values[1::2], 1), 1)
    return [added(left, right) for left, right in zip(even, odd)]


def setup_kernel(begins, green_ref, factor_ref, col_ref, inv_ref, row_ref, spec_ref,
                 wide_ref, green_vm, factor_vm, sem):
    extent = col_ref.shape[1]
    half = extent // 2
    eighth = extent // 4
    period = 2 * extent
    first = pltpu.make_async_copy(factor_ref, factor_vm, sem.at[8])
    first.start()
    copies = [
        pltpu.make_async_copy(
            green_ref.at[pl.ds(q * eighth, eighth)], green_vm.at[pl.ds(q * eighth, eighth)], sem.at[q]
        )
        for q in range(8)
    ]
    for copy in copies:
        copy.start()
    first.wait()

    def column_tables(base, i):
        cos_a = factor_vm[begins[base] + i : begins[base] + i + 1, :]
        sin_a = factor_vm[begins[base + 1] + i : begins[base + 1] + i + 1, :]
        cos_b = factor_vm[begins[base + 2] : begins[base + 2] + GROUP, :]
        sin_b = factor_vm[begins[base + 3] : begins[base + 3] + GROUP, :]
        return turned(cos_a, sin_a, cos_b, sin_b)

    parity = lax.broadcasted_iota(jnp.int32, (GROUP, extent), 1) % 2
    flip = jnp.where(parity == 0, 1.0, -1.0)
    for i in range(half // GROUP):
        rows = i * GROUP
        cosine, sine = column_tables(0, i)
        col_ref[rows : rows + GROUP, :] = cosine.astype(jnp.bfloat16)
        col_ref[half + rows : half + rows + GROUP, :] = (-sine).astype(jnp.bfloat16)
        cosine, sine = column_tables(4, i)
        block = rows // eighth * extent + rows % eighth
        for turn in range(2):
            if turn:
                cosine, sine = cosine * flip, sine * flip
            at = block + turn * eighth
            wide_ref[at : at + GROUP, :] = cosine.astype(jnp.bfloat16)
            wide_ref[at + half : at + half + GROUP, :] = (-sine).astype(jnp.bfloat16)
        coarse = factor_vm[begins[8] + i : begins[8] + i + 1, :]
        for turn in range(2):
            fine = factor_vm[begins[9 + turn] : begins[9 + turn] + GROUP, :]
            cosine, sine = turned(coarse[:, :half], coarse[:, half:], fine[:, :half], fine[:, half:])
            at = turn * half + rows
            inv_ref[at : at + GROUP, :half] = cosine.astype(jnp.bfloat16)
            inv_ref[at : at + GROUP, half:] = (-sine).astype(jnp.bfloat16)
    for j in range(8):
        fine = factor_vm[begins[12] + j * GROUP : begins[12] + (j + 1) * GROUP, :]
        for i in range(eighth // GROUP):
            coarse = factor_vm[begins[11] + i : begins[11] + i + 1, :]
            cosine, sine = turned(
                coarse[:, :eighth], coarse[:, eighth:half], fine[:, :eighth], fine[:, eighth:half]
            )
            upper = i * GROUP
            lower = eighth + i * GROUP
            row_ref[j, upper : upper + GROUP, :eighth] = cosine.astype(jnp.bfloat16)
            row_ref[j, upper : upper + GROUP, eighth:] = sine.astype(jnp.bfloat16)
            row_ref[j, lower : lower + GROUP, :eighth] = (-sine).astype(jnp.bfloat16)
            row_ref[j, lower : lower + GROUP, eighth:] = cosine.astype(jnp.bfloat16)

    for copy in copies:
        copy.wait()
    scale = 1.0 / (period * period)
    parity = lax.broadcasted_iota(jnp.int32, (half, eighth), 0) % 2
    sign = jnp.where(parity == 0, 1.0, -1.0)
    for begin in range(0, extent, half):
        table = wide_ref[2 * begin : 2 * begin + extent, :]
        parts = []
        for q in range(8):
            block = green_vm[q * eighth : (q + 1) * eighth, :].astype(jnp.bfloat16)
            near = dot_nt(table, block[:, :extent])
            far = dot_nt(table, block[:, extent:])
            parts.append((near[:half] - sign * far[half:], near[half:] + sign * far[:half]))
        even = four_points([added(parts[q], parts[q + 4]) for q in range(4)], -1)
        odd = four_points(eighths([less(parts[q], parts[q + 4]) for q in range(4)], -1), -1)
        sums = [pair for couple in zip(even, odd) for pair in couple]
        for j in range(8):
            spec = dot_nt(joined(sums[j]), row_ref[j]) * scale
            spec_ref[j, begin : begin + half, :] = spec.astype(jnp.bfloat16)


def codes(cells, half):
    return jnp.where(cells < half, cells, half - 1.0 - cells).astype(jnp.bfloat16)


def row_nodes(extent, width):
    return lax.broadcasted_iota(jnp.int32, (extent, width), 0).astype(jnp.float32)


def column_nodes(extent, width):
    nodes = (2 * lax.broadcasted_iota(jnp.int32, (extent // 2, width), 0)).astype(jnp.float32)
    return jnp.concatenate([nodes, nodes + 1.0], axis=0)


def hats(nodes, position, weight=1.0):
    half = nodes.shape[0] // 2
    cell = jnp.floor(position)
    part = position - cell
    here = codes(nodes, half)
    low = (weight * (1.0 - part)).astype(jnp.bfloat16)
    high = (weight * part).astype(jnp.bfloat16)
    zero = jnp.zeros_like(here)
    above = jnp.where(here == codes(cell + 1.0, half), high, zero)
    return jnp.where(here == codes(cell, half), low, above)


def kicks(guest_rows, guest_cols, guest_charge, rows, cols, col_ref, inv_ref, row_ref, spec_ref, back_ref):
    extent = col_ref.shape[1]
    half = extent // 2
    eighth = extent // 4
    particles = rows.shape[1]
    weight_rows = hats(row_nodes(extent, particles), guest_rows)
    weight_cols = hats(column_nodes(extent, particles), guest_cols, guest_charge)
    grid = dot_nt(weight_cols, weight_rows).astype(jnp.bfloat16)
    for turn in range(2):
        at = turn * eighth
        re_rows = slice(at, at + eighth)
        im_rows = slice(half + at, half + at + eighth)
        table = jnp.concatenate([col_ref[re_rows, :], col_ref[im_rows, :]], axis=0)
        even = dot_nn(table[:, :half], grid[:half])
        odd = dot_nn(table[:, half:], grid[half:])
        plus, minus = even + odd, even - odd
        real = jnp.concatenate([plus[:eighth], minus[:eighth]], axis=0).astype(jnp.bfloat16)
        imag = jnp.concatenate([plus[eighth:], minus[eighth:]], axis=0).astype(jnp.bfloat16)
        blocks = [
            (real[:, q * eighth : (q + 1) * eighth], imag[:, q * eighth : (q + 1) * eighth])
            for q in range(4)
        ]
        here = slice(turn * half, (turn + 1) * half)
        backs = []
        for j, pair in enumerate(spread(blocks)):
            forward = dot_nt(joined(pair), row_ref[j]).astype(jnp.bfloat16)
            kernel_re = spec_ref[j, here, :eighth]
            kernel_im = spec_ref[j, here, eighth:]
            forward_re, forward_im = forward[:, :eighth], forward[:, eighth:]
            scaled = joined(
                (
                    forward_re * kernel_re - forward_im * kernel_im,
                    forward_re * kernel_im + forward_im * kernel_re,
                )
            )
            back = dot_nn(scaled, row_ref[j]).astype(jnp.bfloat16)
            backs.append((back[:, :eighth], back[:, eighth:]))
        for q, pair in enumerate(gathered(backs)):
            lanes = slice(q * eighth, (q + 1) * eighth)
            for value, where in zip(pair, (re_rows, im_rows)):
                low, high = value[:eighth], value[eighth:]
                back_ref[0, where, lanes] = low + high
                back_ref[1, where, lanes] = low - high
    even = dot_nn(inv_ref[:half, :], back_ref[0])
    odd = dot_nn(inv_ref[half:, :], back_ref[1])
    zero_lane = jnp.zeros((extent, 1), jnp.float32)
    zero_row = jnp.zeros((1, extent), jnp.float32)
    potential = jnp.concatenate([even, odd], axis=0)
    before = jnp.concatenate([zero_lane, potential[:, :-1]], axis=1)
    after = jnp.concatenate([potential[:, 1:], zero_lane], axis=1)
    along_rows = (before - after).astype(jnp.bfloat16)
    before = jnp.concatenate([zero_row, odd[:-1]], axis=0)
    after = jnp.concatenate([even[1:], zero_row], axis=0)
    along_cols = jnp.concatenate([before - odd, even - after], axis=0).astype(jnp.bfloat16)
    weight_rows = hats(row_nodes(extent, particles), rows)
    weight_cols = hats(column_nodes(extent, particles), cols)

    def sampled(field):
        terms = dot_nn(field, weight_rows).astype(jnp.bfloat16) * weight_cols
        count = extent
        while count > 16:
            count //= 2
            terms = terms[:count] + terms[count:]
        return jnp.sum(terms.astype(jnp.float32), axis=0, keepdims=True)

    kick_rows = sampled(along_rows)
    kick_cols = sampled(along_cols)
    return kick_rows, kick_cols


def advance(position, moment, extent):
    return jnp.clip(position + DRIFT_STEP * moment, 1.0, extent - 2.0 - 1.0 / 64.0)


def store_moved(out_ref, moment_out_ref, rows, cols, charge, kick_rows, kick_cols, moment_rows, moment_cols, extent):
    moment_rows = moment_rows + kick_rows
    moment_cols = moment_cols + kick_cols
    moment_out_ref[0:1, :] = moment_rows
    moment_out_ref[1:2, :] = moment_cols
    out_ref[0:1, :] = advance(rows, moment_rows, extent)
    out_ref[1:2, :] = advance(cols, moment_cols, extent)
    out_ref[2:3, :] = charge
    out_ref[3:4, :] = charge


def first_kernel(shards, cells_ref, offsets_ref, charges_ref, momenta_ref, *rest):
    received = rest[:-8]
    col_ref, inv_ref, row_ref, spec_ref, out_ref, moment_out_ref, moment_ref, back_ref = rest[-8:]
    extent = col_ref.shape[1]
    shard = lax.axis_index("tr")
    role = lax.rem(shard, 2)
    own, guest = 1 - role, role
    count = momenta_ref.shape[-1]
    if count == moment_ref.shape[-1]:
        moment_ref[...] = momenta_ref[own]
    else:
        for step, piece in enumerate((momenta_ref, *received)):
            source = lax.rem(shard + shards - step, shards)
            begin = pl.multiple_of(source * count, count)
            moment_ref[:, pl.ds(begin, count)] = piece[own]
    own_place = cells_ref[own].astype(jnp.float32) + offsets_ref[own]
    guest_place = cells_ref[guest].astype(jnp.float32) + offsets_ref[guest]
    rows, cols = own_place[0:1], own_place[1:2]
    kick_rows, kick_cols = kicks(
        guest_place[0:1], guest_place[1:2], charges_ref[guest], rows, cols,
        col_ref, inv_ref, row_ref, spec_ref, back_ref,
    )
    store_moved(
        out_ref, moment_out_ref, rows, cols, charges_ref[own], kick_rows, kick_cols,
        moment_ref[0:1, :], moment_ref[1:2, :], extent,
    )


def middle_kernel(guest_ref, own_ref, moment_ref, col_ref, inv_ref, row_ref, spec_ref,
                  out_ref, moment_out_ref, back_ref):
    extent = col_ref.shape[1]
    rows, cols = own_ref[0:1, :], own_ref[1:2, :]
    kick_rows, kick_cols = kicks(
        guest_ref[0:1, :], guest_ref[1:2, :], guest_ref[2:3, :], rows, cols,
        col_ref, inv_ref, row_ref, spec_ref, back_ref,
    )
    store_moved(
        out_ref, moment_out_ref, rows, cols, own_ref[2:3, :], kick_rows, kick_cols,
        moment_ref[0:1, :], moment_ref[1:2, :], extent,
    )


def last_kernel(guest_ref, own_ref, moment_ref, col_ref, inv_ref, row_ref, spec_ref,
                mine_ref, theirs_ref, total_ref, back_ref):
    count = mine_ref.shape[1]
    kick_rows, kick_cols = kicks(
        guest_ref[0:1, :], guest_ref[1:2, :], guest_ref[2:3, :], own_ref[0:1, :], own_ref[1:2, :],
        col_ref, inv_ref, row_ref, spec_ref, back_ref,
    )
    total_ref[0:1, :] = moment_ref[0:1, :] + kick_rows
    total_ref[1:2, :] = moment_ref[1:2, :] + kick_cols
    if count == total_ref.shape[1]:
        mine_ref[...] = total_ref[...]
        theirs_ref[...] = total_ref[...]
        return
    shard = lax.axis_index("tr")
    partner = shard + 1 - 2 * lax.rem(shard, 2)
    mine_ref[...] = total_ref[:, pl.ds(pl.multiple_of(shard * count, count), count)]
    theirs_ref[...] = total_ref[:, pl.ds(pl.multiple_of(partner * count, count), count)]


def per_device(cells, offsets, charges, momenta, green):
    shards = lax.axis_size("tr")
    slices = lax.axis_size("cuts")
    period = green.shape[0]
    extent = period // 2
    particles = cells.shape[-1]
    own_count = momenta.shape[-1]

    def slot(cut, part):
        return (cut % slices) * shards + part

    def exchange(value, steps):
        pairs = []
        for cut in range(slices):
            for part in range(shards):
                turn = steps if part % 2 == 1 else -steps
                pairs.append((slot(cut, part), slot(cut + turn, part ^ 1)))
        return lax.ppermute(value, ("cuts", "tr"), pairs)

    momenta = momenta[:, 0]
    received = [
        lax.ppermute(momenta, "tr", [(i, (i + step) % shards) for i in range(shards)])
        for step in range(1, shards)
    ]
    aligned = own_count % 128 == 0
    shard = lax.axis_index("tr")
    if not aligned:
        momenta = jnp.concatenate([*received[::-1], momenta], axis=2)
        momenta = jnp.roll(momenta, (shard + 1) * own_count, axis=2)
        received = []

    packed, begins = factors(extent)
    tables = pl.pallas_call(
        functools.partial(setup_kernel, begins),
        out_shape=(
            jax.ShapeDtypeStruct((extent, extent), jnp.bfloat16),
            jax.ShapeDtypeStruct((extent, extent), jnp.bfloat16),
            jax.ShapeDtypeStruct((8, extent // 2, extent // 2), jnp.bfloat16),
            jax.ShapeDtypeStruct((8, extent, extent // 2), jnp.bfloat16),
        ),
        in_specs=[HBM, HBM],
        out_specs=(VMEM,) * 4,
        scratch_shapes=[
            pltpu.VMEM((period, extent), jnp.bfloat16),
            pltpu.VMEM((period, period), jnp.float32),
            pltpu.VMEM(packed.shape, jnp.float32),
            pltpu.SemaphoreType.DMA((9,)),
        ],
        compiler_params=pltpu.CompilerParams(vmem_limit_bytes=SETUP_VMEM),
        cost_estimate=pl.CostEstimate(
            flops=3 * period**3, bytes_accessed=8 * period**2, transcendentals=0
        ),
        name="setup",
    )(green, jnp.asarray(packed))

    place = jax.ShapeDtypeStruct((4, particles), jnp.float32)
    moments = jax.ShapeDtypeStruct((2, particles), jnp.float32)
    piece = jax.ShapeDtypeStruct((2, own_count), jnp.float32)
    back = pltpu.VMEM((2, extent, extent), jnp.bfloat16)
    whole = pltpu.VMEM((2, particles), jnp.float32)

    def section(kernel, name, outs, scratch, arguments):
        return pl.pallas_call(
            kernel,
            out_shape=outs,
            in_specs=[VMEM] * (len(arguments) + 4),
            out_specs=(VMEM,) * len(outs),
            scratch_shapes=scratch,
            compiler_params=pltpu.CompilerParams(vmem_limit_bytes=SECTION_VMEM),
            cost_estimate=pl.CostEstimate(
                flops=3 * period**3, bytes_accessed=8 * period**2, transcendentals=0
            ),
            name=name,
        )(*arguments, *tables)

    own, moment = section(
        functools.partial(first_kernel, shards), "first", (place, moments), [whole, back],
        (cells[:, 0], offsets[:, 0], charges, momenta, *received),
    )
    for number in range(1, SECTIONS - 1):
        guest = exchange(own, 2 * number)
        own, moment = section(middle_kernel, "middle", (place, moments), [back], (guest, own, moment))
    guest = exchange(own, 2 * (SECTIONS - 1))
    role = shard % 2
    outs = (piece, piece) if aligned else (moments, moments)
    mine, theirs = section(last_kernel, "last", outs, [whole, back], (guest, own, moment))
    if not aligned:
        theirs = lax.dynamic_slice_in_dim(mine, (shard + 1 - 2 * role) * own_count, own_count, axis=1)
        mine = lax.dynamic_slice_in_dim(mine, shard * own_count, own_count, axis=1)
    received = exchange(theirs, 0)
    first = jnp.where(role == 1, mine, received)
    second = jnp.where(role == 1, received, mine)
    return jnp.stack([first, second])[:, None]


def solution(mesh):
    return jax.shard_map(
        per_device,
        mesh=mesh,
        in_specs=(
            P(None, "cuts", None, None),
            P(None, "cuts", None, None),
            P(None, "cuts", None),
            P(None, "cuts", None, "tr"),
            P(),
        ),
        out_specs=P(None, "cuts", None, "tr"),
        check_vma=False,
    )
```

```python
import functools
import math

import jax
import jax.numpy as jnp
import numpy as np
from jax import lax
from jax.experimental import pallas as pl
from jax.experimental.pallas import tpu as pltpu
from jax.sharding import PartitionSpec as P

SECTIONS = 4
DRIFT_STEP = 0.5
GROUP = 16
SETUP_VMEM = 32 * 1024 * 1024
WEIGHTS_VMEM = 16 * 1024 * 1024
SECTION_VMEM = 28 * 1024 * 1024
HALF_ROOT = math.sqrt(0.5)

VMEM = pl.BlockSpec(memory_space=pltpu.VMEM)
HBM = pl.BlockSpec(memory_space=pltpu.MemorySpace.HBM)


def dot_nn(left, right):
    return jnp.dot(left, right, preferred_element_type=jnp.float32)


def dot_nt(left, right):
    return lax.dot_general(
        left, right, (((1,), (1,)), ((), ())), preferred_element_type=jnp.float32
    )


def phases(products, period):
    theta = 2.0 * np.pi / period * (products % period)
    return np.cos(theta).astype(np.float32), np.sin(theta).astype(np.float32)


def factors(extent):
    half = extent // 2
    eighth = extent // 4
    period = 2 * extent
    cells = np.arange(extent, dtype=np.int64)
    split = np.concatenate([cells[0::2], cells[1::2]])
    odd = 2 * cells[:half] + 1
    fine = np.arange(GROUP, dtype=np.int64)
    coarse = np.arange(half // GROUP, dtype=np.int64)
    few = np.arange(eighth // GROUP, dtype=np.int64)
    starts = (8 * fine[None, :] + np.arange(8)[:, None]).reshape(-1)
    pieces = []
    pieces += phases(2 * GROUP * coarse[:, None] * split[None, :], 2 * period)
    pieces += phases((2 * fine + 1)[:, None] * split[None, :], 2 * period)
    for rows in (2 * GROUP * coarse, 2 * fine, 2 * fine + 1):
        pieces.append(np.concatenate(phases(rows[:, None] * odd[None, :], 2 * period), axis=1))
    for rows in (8 * GROUP * few, starts):
        both = np.concatenate(phases(rows[:, None] * cells[None, :eighth], period), axis=1)
        pieces.append(np.concatenate([both, both], axis=1))
    begins = np.cumsum([0] + [piece.shape[0] for piece in pieces])
    total = -(-int(begins[-1]) // 8) * 8
    packed = np.zeros((total, extent), np.float32)
    packed[: begins[-1]] = np.concatenate(pieces, axis=0)
    return packed, [int(begin) for begin in begins[:-1]]


def turned(cos_a, sin_a, cos_b, sin_b):
    return cos_a * cos_b - sin_a * sin_b, sin_a * cos_b + cos_a * sin_b


def added(left, right):
    return left[0] + right[0], left[1] + right[1]


def less(left, right):
    return left[0] - right[0], left[1] - right[1]


def times_i(value):
    return -value[1], value[0]


def four_points(values, turn):
    even, even_less = added(values[0], values[2]), less(values[0], values[2])
    odd, odd_less = added(values[1], values[3]), less(values[1], values[3])
    side = times_i(odd_less)
    up, down = added(even_less, side), less(even_less, side)
    if turn < 0:
        up, down = down, up
    return added(even, odd), up, less(even, odd), down


def eighths(values, turn):
    first, second, third, fourth = values
    plus = ((second[0] - turn * second[1]) * HALF_ROOT, (second[1] + turn * second[0]) * HALF_ROOT)
    third = times_i(third)
    if turn < 0:
        third = (-third[0], -third[1])
    minus = (
        (-fourth[0] - turn * fourth[1]) * HALF_ROOT,
        (turn * fourth[0] - fourth[1]) * HALF_ROOT,
    )
    return first, plus, third, minus


def joined(pair):
    return jnp.concatenate([pair[0].astype(jnp.bfloat16), pair[1].astype(jnp.bfloat16)], axis=1)


def spread(values):
    even = four_points(values, -1)
    odd = four_points(eighths(values, -1), -1)
    return [pair for couple in zip(even, odd) for pair in couple]


def gathered(values):
    even = four_points(values[0::2], 1)
    odd = eighths(four_points(values[1::2], 1), 1)
    return [added(left, right) for left, right in zip(even, odd)]


def setup_kernel(begins, green_ref, factor_ref, cells_ref, offsets_ref,
                 col_ref, inv_ref, row_ref, spec_ref, even_ref, slope_ref, split_ref,
                 green_vm, factor_vm, cells_vm, offsets_vm, sem):
    extent = col_ref.shape[1]
    half = extent // 2
    eighth = extent // 4
    period = 2 * extent
    small = [
        pltpu.make_async_copy(source, target, sem.at[8 + number])
        for number, (source, target) in enumerate(
            [(cells_ref, cells_vm), (offsets_ref, offsets_vm), (factor_ref, factor_vm)]
        )
    ]
    for copy in small:
        copy.start()
    copies = [
        pltpu.make_async_copy(
            green_ref.at[:, pl.ds(b * eighth, eighth)], green_vm.at[b], sem.at[b]
        )
        for b in range(8)
    ]
    for copy in copies:
        copy.start()
    own = 1 - lax.rem(lax.axis_index("tr"), 2)
    small[0].wait()
    small[1].wait()
    place = cells_vm[own].astype(jnp.float32) + offsets_vm[own]
    store_weights(place, even_ref, slope_ref, split_ref)
    small[2].wait()

    for i in range(half // GROUP):
        rows = i * GROUP
        cosine, sine = turned(
            factor_vm[begins[0] + i : begins[0] + i + 1, :],
            factor_vm[begins[1] + i : begins[1] + i + 1, :],
            factor_vm[begins[2] : begins[2] + GROUP, :],
            factor_vm[begins[3] : begins[3] + GROUP, :],
        )
        col_ref[rows : rows + GROUP, :] = cosine.astype(jnp.bfloat16)
        col_ref[half + rows : half + rows + GROUP, :] = (-sine).astype(jnp.bfloat16)
        coarse = factor_vm[begins[4] + i : begins[4] + i + 1, :]
        for turn in range(2):
            fine = factor_vm[begins[5 + turn] : begins[5 + turn] + GROUP, :]
            cosine, sine = turned(coarse[:, :half], coarse[:, half:], fine[:, :half], fine[:, half:])
            at = turn * half + rows
            inv_ref[at : at + GROUP, :half] = cosine.astype(jnp.bfloat16)
            inv_ref[at : at + GROUP, half:] = (-sine).astype(jnp.bfloat16)
    for j in range(8):
        fine = factor_vm[begins[8] + j * GROUP : begins[8] + (j + 1) * GROUP, :]
        for i in range(eighth // GROUP):
            coarse = factor_vm[begins[7] + i : begins[7] + i + 1, :]
            cosine, sine = turned(
                coarse[:, :eighth], coarse[:, eighth:half], fine[:, :eighth], fine[:, eighth:half]
            )
            upper = i * GROUP
            lower = eighth + i * GROUP
            row_ref[j, upper : upper + GROUP, :eighth] = cosine.astype(jnp.bfloat16)
            row_ref[j, upper : upper + GROUP, eighth:] = sine.astype(jnp.bfloat16)
            row_ref[j, lower : lower + GROUP, :eighth] = (-sine).astype(jnp.bfloat16)
            row_ref[j, lower : lower + GROUP, eighth:] = cosine.astype(jnp.bfloat16)

    scale = 1.0 / (period * period)
    parity = lax.broadcasted_iota(jnp.int32, (half, eighth), 0) % 2
    sign = jnp.where(parity == 0, 1.0, -1.0)
    parts = [[], []]
    for b in range(4):
        copies[2 * b].wait()
        copies[2 * b + 1].wait()
        blocks = [
            joined([green_vm[2 * b + q, pl.ds(begin, half, stride=2), :] for q in range(2)])
            for begin in (0, 1, extent, extent + 1)
        ]
        for turn in range(2):
            table = frequency_rows(col_ref, turn)
            near = both_halves(table, blocks[0], blocks[1])
            far = both_halves(table, blocks[2], blocks[3])
            for q in range(2):
                cut = slice(q * eighth, (q + 1) * eighth)
                parts[turn].append(
                    (
                        near[0][:, cut] - sign * far[1][:, cut],
                        near[1][:, cut] + sign * far[0][:, cut],
                    )
                )
    for turn in range(2):
        part = parts[turn]
        even = four_points([added(part[q], part[q + 4]) for q in range(4)], -1)
        odd = four_points(eighths([less(part[q], part[q + 4]) for q in range(4)], -1), -1)
        sums = [pair for couple in zip(even, odd) for pair in couple]
        for j in range(8):
            spec = dot_nt(joined(sums[j]), row_ref[j]) * scale
            spec_ref[j, turn * half : (turn + 1) * half, :] = spec.astype(jnp.bfloat16)


def frequency_rows(col_ref, turn):
    half = col_ref.shape[0] // 2
    eighth = half // 2
    at = turn * eighth
    return jnp.concatenate(
        [col_ref[at : at + eighth, :], col_ref[half + at : half + at + eighth, :]], axis=0
    )


def both_halves(table, even_rows, odd_rows):
    half = table.shape[1] // 2
    eighth = half // 2
    even = dot_nn(table[:, :half], even_rows)
    odd = dot_nn(table[:, half:], odd_rows)
    plus, minus = even + odd, even - odd
    return (
        jnp.concatenate([plus[:eighth], minus[:eighth]], axis=0),
        jnp.concatenate([plus[eighth:], minus[eighth:]], axis=0),
    )


def codes(cells, half):
    return jnp.where(cells < half, cells, half - 1.0 - cells)


def chosen(extent, split, pairs):
    half = extent // 2
    width = pairs[0][0].shape[1]

    def raised(row):
        return jnp.broadcast_to(row, (GROUP, width)).astype(jnp.bfloat16)

    cells = [raised(codes(cell, half)) for cell, _ in pairs]
    weights = [raised(weight) for _, weight in pairs]
    count = lax.broadcasted_iota(jnp.int32, (GROUP, width), 0)
    blocks = []
    for begin in range(0, extent, GROUP):
        if split:
            nodes = 2 * (begin % half) + begin // half + 2 * count
        else:
            nodes = begin + count
        here = codes(nodes.astype(jnp.float32), half).astype(jnp.bfloat16)
        result = jnp.zeros_like(here)
        for cell, weight in zip(reversed(cells), reversed(weights)):
            result = jnp.where(here == cell, weight, result)
        blocks.append(result)
    return jnp.concatenate(blocks, axis=0)


def parted(position):
    cell = jnp.floor(position)
    return cell, position - cell


def hats(extent, split, position, weight=1.0):
    cell, part = parted(position)
    return chosen(extent, split, [(cell, weight * (1.0 - part)), (cell + 1.0, weight * part)])


def slopes(extent, position):
    cell, part = parted(position)
    return chosen(
        extent,
        False,
        [(cell - 1.0, 1.0 - part), (cell, part), (cell + 1.0, part - 1.0), (cell + 2.0, -part)],
    )


def store_weights(place, even_ref, slope_ref, split_ref):
    extent = even_ref.shape[0]
    even_ref[...] = hats(extent, False, place[1:2])
    slope_ref[...] = slopes(extent, place[1:2])
    split_ref[...] = hats(extent, True, place[0:1])


def weights_kernel(own_ref, even_ref, slope_ref, split_ref):
    store_weights(own_ref[0:2, :], even_ref, slope_ref, split_ref)


def kicks(guest, charge, even_ref, slope_ref, split_ref, col_ref, inv_ref, row_ref, spec_ref, back_ref):
    extent = col_ref.shape[1]
    half = extent // 2
    eighth = extent // 4
    weights_second = hats(extent, False, guest[1:2])
    weights_first = hats(extent, True, guest[0:1], charge)
    grid = dot_nt(weights_first, weights_second).astype(jnp.bfloat16)
    spreads = []
    for turn in range(2):
        real, imag = both_halves(frequency_rows(col_ref, turn), grid[:half], grid[half:])
        real, imag = real.astype(jnp.bfloat16), imag.astype(jnp.bfloat16)
        blocks = [
            (real[:, q * eighth : (q + 1) * eighth], imag[:, q * eighth : (q + 1) * eighth])
            for q in range(4)
        ]
        spreads.append(spread(blocks))
    for turn in range(2):
        here = slice(turn * half, (turn + 1) * half)
        backs = []
        for j, pair in enumerate(spreads[turn]):
            forward = dot_nt(joined(pair), row_ref[j]).astype(jnp.bfloat16)
            kernel_re = spec_ref[j, here, :eighth]
            kernel_im = spec_ref[j, here, eighth:]
            forward_re, forward_im = forward[:, :eighth], forward[:, eighth:]
            scaled = joined(
                (
                    forward_re * kernel_re - forward_im * kernel_im,
                    forward_re * kernel_im + forward_im * kernel_re,
                )
            )
            back = dot_nn(scaled, row_ref[j]).astype(jnp.bfloat16)
            backs.append((back[:, :eighth], back[:, eighth:]))
        for q, pair in enumerate(gathered(backs)):
            lanes = slice(q * eighth, (q + 1) * eighth)
            for part, value in enumerate(pair):
                where = slice(part * half + turn * eighth, part * half + (turn + 1) * eighth)
                low, high = value[:eighth], value[eighth:]
                back_ref[0, where, lanes] = low + high
                back_ref[1, where, lanes] = low - high
    even = dot_nn(inv_ref[:half, :], back_ref[0])
    odd = dot_nn(inv_ref[half:, :], back_ref[1])
    zero_row = jnp.zeros((1, extent), jnp.float32)
    before = jnp.concatenate([zero_row, odd[:-1]], axis=0)
    after = jnp.concatenate([even[1:], zero_row], axis=0)
    field = jnp.concatenate([before - odd, even - after], axis=0).astype(jnp.bfloat16)
    potential = jnp.concatenate([even, odd], axis=0).astype(jnp.bfloat16)

    def sampled(values, weights_ref):
        terms = dot_nn(values, weights_ref[...]).astype(jnp.bfloat16) * split_ref[...]
        count = extent
        while count > 16:
            count //= 2
            terms = terms[:count] + terms[count:]
        return jnp.sum(terms.astype(jnp.float32), axis=0, keepdims=True)

    return sampled(field, even_ref), sampled(potential, slope_ref)


def advance(position, moment, extent):
    return jnp.clip(position + DRIFT_STEP * moment, 1.0, extent - 2.0 - 1.0 / 64.0)


def store_moved(out_ref, moment_out_ref, place, charge, kick, moment, extent):
    for dim in range(2):
        line = slice(dim, dim + 1)
        total = moment[line] + kick[dim]
        moment_out_ref[line, :] = total
        out_ref[line, :] = advance(place[line], total, extent)
    out_ref[2:3, :] = charge
    out_ref[3:4, :] = charge


def first_kernel(shards, cells_ref, offsets_ref, charges_ref, momenta_ref, *rest):
    received = rest[:-11]
    common = rest[-11:-4]
    out_ref, moment_out_ref, moment_ref, back_ref = rest[-4:]
    shard = lax.axis_index("tr")
    role = lax.rem(shard, 2)
    own, guest = 1 - role, role
    count = momenta_ref.shape[-1]
    if count == moment_ref.shape[-1]:
        moment_ref[...] = momenta_ref[own]
    else:
        for step, piece in enumerate((momenta_ref, *received)):
            source = lax.rem(shard + shards - step, shards)
            begin = pl.multiple_of(source * count, count)
            moment_ref[:, pl.ds(begin, count)] = piece[own]
    own_place = cells_ref[own].astype(jnp.float32) + offsets_ref[own]
    guest_place = cells_ref[guest].astype(jnp.float32) + offsets_ref[guest]
    kick = kicks(guest_place, charges_ref[guest], *common, back_ref)
    extent = common[0].shape[0]
    store_moved(out_ref, moment_out_ref, own_place, charges_ref[own], kick, moment_ref[...], extent)


def middle_kernel(guest_ref, own_ref, moment_ref, *rest):
    common = rest[:7]
    out_ref, moment_out_ref, back_ref = rest[7:]
    kick = kicks(guest_ref[0:2, :], guest_ref[2:3, :], *common, back_ref)
    own, extent = own_ref[...], common[0].shape[0]
    store_moved(out_ref, moment_out_ref, own[0:2], own[2:3], kick, moment_ref[...], extent)


def last_kernel(guest_ref, moment_ref, *rest):
    common = rest[:7]
    mine_ref, theirs_ref, total_ref, back_ref = rest[7:]
    count = mine_ref.shape[1]
    kick = kicks(guest_ref[0:2, :], guest_ref[2:3, :], *common, back_ref)
    total_ref[0:1, :] = moment_ref[0:1, :] + kick[0]
    total_ref[1:2, :] = moment_ref[1:2, :] + kick[1]
    if count == total_ref.shape[1]:
        mine_ref[...] = total_ref[...]
        theirs_ref[...] = total_ref[...]
        return
    shard = lax.axis_index("tr")
    partner = shard + 1 - 2 * lax.rem(shard, 2)
    mine_ref[...] = total_ref[:, pl.ds(pl.multiple_of(shard * count, count), count)]
    theirs_ref[...] = total_ref[:, pl.ds(pl.multiple_of(partner * count, count), count)]


def per_device(cells, offsets, charges, momenta, green):
    shards = lax.axis_size("tr")
    slices = lax.axis_size("cuts")
    period = green.shape[0]
    extent = period // 2
    particles = cells.shape[-1]
    own_count = momenta.shape[-1]

    def slot(cut, part):
        return (cut % slices) * shards + part

    def exchange(value, steps):
        pairs = []
        for cut in range(slices):
            for part in range(shards):
                turn = steps if part % 2 == 1 else -steps
                pairs.append((slot(cut, part), slot(cut + turn, part ^ 1)))
        return lax.ppermute(value, ("cuts", "tr"), pairs)

    momenta = momenta[:, 0]
    received = [
        lax.ppermute(momenta, "tr", [(i, (i + step) % shards) for i in range(shards)])
        for step in range(1, shards)
    ]
    aligned = own_count % 128 == 0
    shard = lax.axis_index("tr")
    if not aligned:
        momenta = jnp.concatenate([*received[::-1], momenta], axis=2)
        momenta = jnp.roll(momenta, (shard + 1) * own_count, axis=2)
        received = []

    packed, begins = factors(extent)
    weight = jax.ShapeDtypeStruct((extent, particles), jnp.bfloat16)
    *tables, even, slope, split = pl.pallas_call(
        functools.partial(setup_kernel, begins),
        out_shape=(
            jax.ShapeDtypeStruct((extent, extent), jnp.bfloat16),
            jax.ShapeDtypeStruct((extent, extent), jnp.bfloat16),
            jax.ShapeDtypeStruct((8, extent // 2, extent // 2), jnp.bfloat16),
            jax.ShapeDtypeStruct((8, extent, extent // 2), jnp.bfloat16),
            weight, weight, weight,
        ),
        in_specs=[HBM] * 4,
        out_specs=(VMEM,) * 7,
        scratch_shapes=[
            pltpu.VMEM((8, period, extent // 4), jnp.float32),
            pltpu.VMEM(packed.shape, jnp.float32),
            pltpu.VMEM((2, 2, particles), jnp.int32),
            pltpu.VMEM((2, 2, particles), jnp.float32),
            pltpu.SemaphoreType.DMA((11,)),
        ],
        compiler_params=pltpu.CompilerParams(vmem_limit_bytes=SETUP_VMEM),
        cost_estimate=pl.CostEstimate(
            flops=2 * period**3, bytes_accessed=8 * period**2, transcendentals=0
        ),
        name="setup",
    )(*[
        pltpu.with_memory_space_constraint(value, pltpu.MemorySpace.HBM)
        for value in (green, jnp.asarray(packed), cells[:, 0], offsets[:, 0])
    ])

    place = jax.ShapeDtypeStruct((4, particles), jnp.float32)
    moments = jax.ShapeDtypeStruct((2, particles), jnp.float32)
    piece = jax.ShapeDtypeStruct((2, own_count), jnp.float32)
    back = pltpu.VMEM((2, extent, extent), jnp.bfloat16)
    whole = pltpu.VMEM((2, particles), jnp.float32)

    def weights(own):
        return pl.pallas_call(
            weights_kernel,
            out_shape=(weight,) * 3,
            in_specs=[VMEM],
            out_specs=(VMEM,) * 3,
            compiler_params=pltpu.CompilerParams(vmem_limit_bytes=WEIGHTS_VMEM),
            cost_estimate=pl.CostEstimate(
                flops=period**3 // 2, bytes_accessed=6 * period**2, transcendentals=0
            ),
            name="weights",
        )(own)

    def section(kernel, name, outs, scratch, arguments):
        return pl.pallas_call(
            kernel,
            out_shape=outs,
            in_specs=[VMEM] * (len(arguments) + 4),
            out_specs=(VMEM,) * len(outs),
            scratch_shapes=scratch,
            compiler_params=pltpu.CompilerParams(vmem_limit_bytes=SECTION_VMEM),
            cost_estimate=pl.CostEstimate(
                flops=3 * period**3, bytes_accessed=8 * period**2, transcendentals=0
            ),
            name=name,
        )(*arguments, *tables)

    own, moment = section(
        functools.partial(first_kernel, shards), "first", (place, moments), [whole, back],
        (cells[:, 0], offsets[:, 0], charges, momenta, *received, even, slope, split),
    )
    for number in range(1, SECTIONS - 1):
        guest = exchange(own, 2 * number)
        own, moment = section(
            middle_kernel, "middle", (place, moments), [back], (guest, own, moment, *weights(own))
        )
    guest = exchange(own, 2 * (SECTIONS - 1))
    role = shard % 2
    outs = (piece, piece) if aligned else (moments, moments)
    mine, theirs = section(
        last_kernel, "last", outs, [whole, back], (guest, moment, *weights(own))
    )
    if not aligned:
        theirs = lax.dynamic_slice_in_dim(mine, (shard + 1 - 2 * role) * own_count, own_count, axis=1)
        mine = lax.dynamic_slice_in_dim(mine, shard * own_count, own_count, axis=1)
    received = exchange(theirs, 0)
    first = jnp.where(role == 1, mine, received)
    second = jnp.where(role == 1, received, mine)
    return jnp.stack([first, second])[:, None]


def solution(mesh):
    return jax.shard_map(
        per_device,
        mesh=mesh,
        in_specs=(
            P(None, "cuts", None, None),
            P(None, "cuts", None, None),
            P(None, "cuts", None),
            P(None, "cuts", None, "tr"),
            P(),
        ),
        out_specs=P(None, "cuts", None, "tr"),
        check_vma=False,
    )
```

```python
import functools
import math

import jax
import jax.numpy as jnp
import numpy as np
from jax import lax
from jax.experimental import pallas as pl
from jax.experimental.pallas import tpu as pltpu
from jax.sharding import PartitionSpec as P

SECTIONS = 4
DRIFT_STEP = 0.5
GROUP = 16
SETUP_VMEM = 32 * 1024 * 1024
WEIGHTS_VMEM = 16 * 1024 * 1024
SECTION_VMEM = 28 * 1024 * 1024
HALF_ROOT = math.sqrt(0.5)

VMEM = pl.BlockSpec(memory_space=pltpu.VMEM)
HBM = pl.BlockSpec(memory_space=pltpu.MemorySpace.HBM)


def dot_nn(left, right):
    return jnp.dot(left, right, preferred_element_type=jnp.float32)


def dot_nt(left, right):
    return lax.dot_general(
        left, right, (((1,), (1,)), ((), ())), preferred_element_type=jnp.float32
    )


def phases(products, period):
    theta = 2.0 * np.pi / period * (products % period)
    return np.cos(theta).astype(np.float32), np.sin(theta).astype(np.float32)


def factors(extent):
    half = extent // 2
    eighth = extent // 4
    period = 2 * extent
    cells = np.arange(extent, dtype=np.int64)
    split = np.concatenate([cells[0::2], cells[1::2]])
    odd = 2 * cells[:half] + 1
    fine = np.arange(GROUP, dtype=np.int64)
    coarse = np.arange(half // GROUP, dtype=np.int64)
    few = np.arange(eighth // GROUP, dtype=np.int64)
    starts = (8 * fine[None, :] + np.arange(8)[:, None]).reshape(-1)
    pieces = []
    pieces += phases(2 * GROUP * coarse[:, None] * split[None, :], 2 * period)
    pieces += phases((2 * fine + 1)[:, None] * split[None, :], 2 * period)
    for rows in (2 * GROUP * coarse, 2 * fine, 2 * fine + 1):
        pieces.append(np.concatenate(phases(rows[:, None] * odd[None, :], 2 * period), axis=1))
    for rows in (8 * GROUP * few, starts):
        both = np.concatenate(phases(rows[:, None] * cells[None, :eighth], period), axis=1)
        pieces.append(np.concatenate([both, both], axis=1))
    begins = np.cumsum([0] + [piece.shape[0] for piece in pieces])
    total = -(-int(begins[-1]) // 8) * 8
    packed = np.zeros((total, extent), np.float32)
    packed[: begins[-1]] = np.concatenate(pieces, axis=0)
    return packed, [int(begin) for begin in begins[:-1]]


def turned(cos_a, sin_a, cos_b, sin_b):
    return cos_a * cos_b - sin_a * sin_b, sin_a * cos_b + cos_a * sin_b


def added(left, right):
    return left[0] + right[0], left[1] + right[1]


def less(left, right):
    return left[0] - right[0], left[1] - right[1]


def times_i(value):
    return -value[1], value[0]


def four_points(values, turn):
    even, even_less = added(values[0], values[2]), less(values[0], values[2])
    odd, odd_less = added(values[1], values[3]), less(values[1], values[3])
    side = times_i(odd_less)
    up, down = added(even_less, side), less(even_less, side)
    if turn < 0:
        up, down = down, up
    return added(even, odd), up, less(even, odd), down


def eighths(values, turn):
    first, second, third, fourth = values
    plus = ((second[0] - turn * second[1]) * HALF_ROOT, (second[1] + turn * second[0]) * HALF_ROOT)
    third = times_i(third)
    if turn < 0:
        third = (-third[0], -third[1])
    minus = (
        (-fourth[0] - turn * fourth[1]) * HALF_ROOT,
        (turn * fourth[0] - fourth[1]) * HALF_ROOT,
    )
    return first, plus, third, minus


def joined(pair):
    return jnp.concatenate([pair[0].astype(jnp.bfloat16), pair[1].astype(jnp.bfloat16)], axis=1)


def spread(values):
    even = four_points(values, -1)
    odd = four_points(eighths(values, -1), -1)
    return [pair for couple in zip(even, odd) for pair in couple]


def gathered(values):
    even = four_points(values[0::2], 1)
    odd = eighths(four_points(values[1::2], 1), 1)
    return [added(left, right) for left, right in zip(even, odd)]


def places_along(shard):
    copy, side = shard // 2, shard % 2
    return copy, side, (side + copy) % 2


def my_place():
    shard = lax.axis_index("tr")
    copy = lax.div(shard, 2)
    side = lax.rem(shard, 2)
    return copy, side, lax.rem(side + copy, 2)


def setup_kernel(begins, green_ref, factor_ref, cells_ref, offsets_ref,
                 col_ref, inv_ref, row_ref, spec_ref, even_ref, slope_ref, split_ref,
                 green_vm, factor_vm, cells_vm, offsets_vm, sem):
    extent = col_ref.shape[1]
    half = extent // 2
    eighth = extent // 4
    period = 2 * extent
    small = [
        pltpu.make_async_copy(source, target, sem.at[8 + number])
        for number, (source, target) in enumerate(
            [(cells_ref, cells_vm), (offsets_ref, offsets_vm), (factor_ref, factor_vm)]
        )
    ]
    for copy in small:
        copy.start()
    copies = [
        pltpu.make_async_copy(
            green_ref.at[:, pl.ds(b * eighth, eighth)], green_vm.at[b], sem.at[b]
        )
        for b in range(8)
    ]
    for copy in copies:
        copy.start()
    copy_index, _, role = my_place()
    own = 1 - role
    small[0].wait()
    small[1].wait()
    width = even_ref.shape[1]
    lanes = pl.ds(pl.multiple_of(copy_index * width, width), width)
    place = cells_vm[own, :, lanes].astype(jnp.float32) + offsets_vm[own, :, lanes]
    store_weights(place, even_ref, slope_ref, split_ref)
    small[2].wait()

    for i in range(half // GROUP):
        rows = i * GROUP
        cosine, sine = turned(
            factor_vm[begins[0] + i : begins[0] + i + 1, :],
            factor_vm[begins[1] + i : begins[1] + i + 1, :],
            factor_vm[begins[2] : begins[2] + GROUP, :],
            factor_vm[begins[3] : begins[3] + GROUP, :],
        )
        col_ref[rows : rows + GROUP, :] = cosine.astype(jnp.bfloat16)
        col_ref[half + rows : half + rows + GROUP, :] = (-sine).astype(jnp.bfloat16)
        coarse = factor_vm[begins[4] + i : begins[4] + i + 1, :]
        for turn in range(2):
            fine = factor_vm[begins[5 + turn] : begins[5 + turn] + GROUP, :]
            cosine, sine = turned(coarse[:, :half], coarse[:, half:], fine[:, :half], fine[:, half:])
            at = turn * half + rows
            inv_ref[at : at + GROUP, :half] = cosine.astype(jnp.bfloat16)
            inv_ref[at : at + GROUP, half:] = (-sine).astype(jnp.bfloat16)
    for j in range(8):
        fine = factor_vm[begins[8] + j * GROUP : begins[8] + (j + 1) * GROUP, :]
        for i in range(eighth // GROUP):
            coarse = factor_vm[begins[7] + i : begins[7] + i + 1, :]
            cosine, sine = turned(
                coarse[:, :eighth], coarse[:, eighth:half], fine[:, :eighth], fine[:, eighth:half]
            )
            upper = i * GROUP
            lower = eighth + i * GROUP
            row_ref[j, upper : upper + GROUP, :eighth] = cosine.astype(jnp.bfloat16)
            row_ref[j, upper : upper + GROUP, eighth:] = sine.astype(jnp.bfloat16)
            row_ref[j, lower : lower + GROUP, :eighth] = (-sine).astype(jnp.bfloat16)
            row_ref[j, lower : lower + GROUP, eighth:] = cosine.astype(jnp.bfloat16)

    scale = 1.0 / (period * period)
    parity = lax.broadcasted_iota(jnp.int32, (half, eighth), 0) % 2
    sign = jnp.where(parity == 0, 1.0, -1.0)
    parts = [[], []]
    for b in range(4):
        copies[2 * b].wait()
        copies[2 * b + 1].wait()
        blocks = [
            joined([green_vm[2 * b + q, pl.ds(begin, half, stride=2), :] for q in range(2)])
            for begin in (0, 1, extent, extent + 1)
        ]
        for turn in range(2):
            table = frequency_rows(col_ref, turn)
            near = both_halves(table, blocks[0], blocks[1])
            far = both_halves(table, blocks[2], blocks[3])
            for q in range(2):
                cut = slice(q * eighth, (q + 1) * eighth)
                parts[turn].append(
                    (
                        near[0][:, cut] - sign * far[1][:, cut],
                        near[1][:, cut] + sign * far[0][:, cut],
                    )
                )
    for turn in range(2):
        part = parts[turn]
        even = four_points([added(part[q], part[q + 4]) for q in range(4)], -1)
        odd = four_points(eighths([less(part[q], part[q + 4]) for q in range(4)], -1), -1)
        sums = [pair for couple in zip(even, odd) for pair in couple]
        for j in range(8):
            spec = dot_nt(joined(sums[j]), row_ref[j]) * scale
            spec_ref[j, turn * half : (turn + 1) * half, :] = spec.astype(jnp.bfloat16)


def frequency_rows(col_ref, turn):
    half = col_ref.shape[0] // 2
    eighth = half // 2
    at = turn * eighth
    return jnp.concatenate(
        [col_ref[at : at + eighth, :], col_ref[half + at : half + at + eighth, :]], axis=0
    )


def both_halves(table, even_rows, odd_rows):
    half = table.shape[1] // 2
    eighth = half // 2
    even = dot_nn(table[:, :half], even_rows)
    odd = dot_nn(table[:, half:], odd_rows)
    plus, minus = even + odd, even - odd
    return (
        jnp.concatenate([plus[:eighth], minus[:eighth]], axis=0),
        jnp.concatenate([plus[eighth:], minus[eighth:]], axis=0),
    )


def codes(cells, half):
    return jnp.where(cells < half, cells, half - 1.0 - cells)


def chosen(extent, split, pairs):
    half = extent // 2
    width = pairs[0][0].shape[1]

    def raised(row):
        return jnp.broadcast_to(row, (GROUP, width)).astype(jnp.bfloat16)

    cells = [raised(codes(cell, half)) for cell, _ in pairs]
    weights = [raised(weight) for _, weight in pairs]
    count = lax.broadcasted_iota(jnp.int32, (GROUP, width), 0)
    blocks = []
    for begin in range(0, extent, GROUP):
        if split:
            nodes = 2 * (begin % half) + begin // half + 2 * count
        else:
            nodes = begin + count
        here = codes(nodes.astype(jnp.float32), half).astype(jnp.bfloat16)
        result = jnp.zeros_like(here)
        for cell, weight in zip(reversed(cells), reversed(weights)):
            result = jnp.where(here == cell, weight, result)
        blocks.append(result)
    return jnp.concatenate(blocks, axis=0)


def parted(position):
    cell = jnp.floor(position)
    return cell, position - cell


def hats(extent, split, position, weight=1.0):
    cell, part = parted(position)
    return chosen(extent, split, [(cell, weight * (1.0 - part)), (cell + 1.0, weight * part)])


def slopes(extent, position):
    cell, part = parted(position)
    return chosen(
        extent,
        False,
        [(cell - 1.0, 1.0 - part), (cell, part), (cell + 1.0, part - 1.0), (cell + 2.0, -part)],
    )


def store_weights(place, even_ref, slope_ref, split_ref):
    extent = even_ref.shape[0]
    even_ref[...] = hats(extent, False, place[1:2])
    slope_ref[...] = slopes(extent, place[1:2])
    split_ref[...] = hats(extent, True, place[0:1])


def deposit(place, charge, extent):
    weights_second = hats(extent, False, place[1:2])
    weights_first = hats(extent, True, place[0:1], charge)
    return dot_nt(weights_first, weights_second)


def deposit_kernel(guest_ref, own_ref, grid_ref, even_ref, slope_ref, split_ref):
    grid_ref[...] = deposit(guest_ref[0:2, :], guest_ref[2:3, :], grid_ref.shape[0])
    store_weights(own_ref[0:2, :], even_ref, slope_ref, split_ref)


def kicks(grid, even_ref, slope_ref, split_ref, col_ref, inv_ref, row_ref, spec_ref, back_ref):
    extent = col_ref.shape[1]
    half = extent // 2
    eighth = extent // 4
    grid = grid.astype(jnp.bfloat16)
    spreads = []
    for turn in range(2):
        real, imag = both_halves(frequency_rows(col_ref, turn), grid[:half], grid[half:])
        real, imag = real.astype(jnp.bfloat16), imag.astype(jnp.bfloat16)
        blocks = [
            (real[:, q * eighth : (q + 1) * eighth], imag[:, q * eighth : (q + 1) * eighth])
            for q in range(4)
        ]
        spreads.append(spread(blocks))
    for turn in range(2):
        here = slice(turn * half, (turn + 1) * half)
        backs = []
        for j, pair in enumerate(spreads[turn]):
            forward = dot_nt(joined(pair), row_ref[j]).astype(jnp.bfloat16)
            kernel_re = spec_ref[j, here, :eighth]
            kernel_im = spec_ref[j, here, eighth:]
            forward_re, forward_im = forward[:, :eighth], forward[:, eighth:]
            scaled = joined(
                (
                    forward_re * kernel_re - forward_im * kernel_im,
                    forward_re * kernel_im + forward_im * kernel_re,
                )
            )
            back = dot_nn(scaled, row_ref[j]).astype(jnp.bfloat16)
            backs.append((back[:, :eighth], back[:, eighth:]))
        for q, pair in enumerate(gathered(backs)):
            lanes = slice(q * eighth, (q + 1) * eighth)
            for part, value in enumerate(pair):
                where = slice(part * half + turn * eighth, part * half + (turn + 1) * eighth)
                low, high = value[:eighth], value[eighth:]
                back_ref[0, where, lanes] = low + high
                back_ref[1, where, lanes] = low - high
    even = dot_nn(inv_ref[:half, :], back_ref[0])
    odd = dot_nn(inv_ref[half:, :], back_ref[1])
    zero_row = jnp.zeros((1, extent), jnp.float32)
    before = jnp.concatenate([zero_row, odd[:-1]], axis=0)
    after = jnp.concatenate([even[1:], zero_row], axis=0)
    field = jnp.concatenate([before - odd, even - after], axis=0).astype(jnp.bfloat16)
    potential = jnp.concatenate([even, odd], axis=0).astype(jnp.bfloat16)

    def sampled(values, weights_ref):
        terms = dot_nn(values, weights_ref[...]).astype(jnp.bfloat16) * split_ref[...]
        count = extent
        while count > 16:
            count //= 2
            terms = terms[:count] + terms[count:]
        return jnp.sum(terms.astype(jnp.float32), axis=0, keepdims=True)

    return sampled(field, even_ref), sampled(potential, slope_ref)


def advance(position, moment, extent):
    return jnp.clip(position + DRIFT_STEP * moment, 1.0, extent - 2.0 - 1.0 / 64.0)


def store_moved(out_ref, moment_out_ref, place, charge, kick, moment, extent):
    for dim in range(2):
        line = slice(dim, dim + 1)
        total = moment[line] + kick[dim]
        moment_out_ref[line, :] = total
        out_ref[line, :] = advance(place[line], total, extent)
    out_ref[2:3, :] = charge
    out_ref[3:4, :] = charge


def first_kernel(cells_ref, offsets_ref, charges_ref, momenta_ref, other_ref, *rest):
    common = rest[:7]
    out_ref, moment_out_ref, back_ref = rest[7:]
    extent, width = common[0].shape
    copy_index, side, role = my_place()
    own, guest = 1 - role, role
    mine, other = momenta_ref[own], other_ref[own]
    moment = jnp.where(
        side == 0, jnp.concatenate([mine, other], axis=1), jnp.concatenate([other, mine], axis=1)
    )
    lanes = pl.ds(pl.multiple_of(copy_index * width, width), width)
    own_place = cells_ref[own, :, lanes].astype(jnp.float32) + offsets_ref[own, :, lanes]
    guest_place = cells_ref[guest].astype(jnp.float32) + offsets_ref[guest]
    grid = deposit(guest_place, charges_ref[guest], extent)
    kick = kicks(grid, *common, back_ref)
    charge = charges_ref[own, :, lanes]
    store_moved(out_ref, moment_out_ref, own_place, charge, kick, moment, extent)


def whole_grid(grid_ref, guest_refs):
    guest = jnp.concatenate([piece[...] for piece in guest_refs], axis=1)
    return grid_ref[...] + deposit(guest[0:2], guest[2:3], grid_ref.shape[0])


def middle_kernel(copies, *refs):
    grid = whole_grid(refs[0], refs[1:copies])
    own_ref, moment_ref = refs[copies : copies + 2]
    common = refs[copies + 2 : copies + 9]
    out_ref, moment_out_ref, back_ref = refs[copies + 9 :]
    kick = kicks(grid, *common, back_ref)
    own, extent = own_ref[...], common[0].shape[0]
    store_moved(out_ref, moment_out_ref, own[0:2], own[2:3], kick, moment_ref[...], extent)


def last_kernel(copies, *refs):
    grid = whole_grid(refs[0], refs[1:copies])
    moment_ref = refs[copies]
    common = refs[copies + 1 : copies + 8]
    mine_ref, theirs_ref, back_ref = refs[copies + 8 :]
    count = mine_ref.shape[1]
    kick = kicks(grid, *common, back_ref)
    total = jnp.concatenate([moment_ref[dim : dim + 1, :] + kick[dim] for dim in range(2)], axis=0)
    low, high = total[:, :count], total[:, count:]
    _, side, _ = my_place()
    mine_ref[...] = jnp.where(side == 0, low, high)
    theirs_ref[...] = jnp.where(side == 0, high, low)


def per_device(cells, offsets, charges, momenta, green):
    shards = lax.axis_size("tr")
    slices = lax.axis_size("cuts")
    period = green.shape[0]
    extent = period // 2
    particles = cells.shape[-1]
    own_count = momenta.shape[-1]

    def slot(cut, part):
        return (cut % slices) * shards + part

    copies = shards // 2

    def exchange(value, steps, further=0):
        pairs = []
        for cut in range(slices):
            for part in range(shards):
                copy, _, role = places_along(part)
                turn = steps if role == 1 else -steps
                goal = (copy + further) % copies
                side = (1 - role + goal) % 2
                pairs.append((slot(cut, part), slot(cut + turn, 2 * goal + side)))
        return lax.ppermute(value, ("cuts", "tr"), pairs)

    momenta = momenta[:, 0]
    other = exchange(momenta, 0)
    packed, begins = factors(extent)
    held = 2 * own_count
    weight = jax.ShapeDtypeStruct((extent, held), jnp.bfloat16)
    *tables, even, slope, split = pl.pallas_call(
        functools.partial(setup_kernel, begins),
        out_shape=(
            jax.ShapeDtypeStruct((extent, extent), jnp.bfloat16),
            jax.ShapeDtypeStruct((extent, extent), jnp.bfloat16),
            jax.ShapeDtypeStruct((8, extent // 2, extent // 2), jnp.bfloat16),
            jax.ShapeDtypeStruct((8, extent, extent // 2), jnp.bfloat16),
            weight, weight, weight,
        ),
        in_specs=[HBM] * 4,
        out_specs=(VMEM,) * 7,
        scratch_shapes=[
            pltpu.VMEM((8, period, extent // 4), jnp.float32),
            pltpu.VMEM(packed.shape, jnp.float32),
            pltpu.VMEM((2, 2, particles), jnp.int32),
            pltpu.VMEM((2, 2, particles), jnp.float32),
            pltpu.SemaphoreType.DMA((11,)),
        ],
        compiler_params=pltpu.CompilerParams(vmem_limit_bytes=SETUP_VMEM),
        cost_estimate=pl.CostEstimate(
            flops=2 * period**3, bytes_accessed=8 * period**2, transcendentals=0
        ),
        name="setup",
    )(*[
        pltpu.with_memory_space_constraint(value, pltpu.MemorySpace.HBM)
        for value in (green, jnp.asarray(packed), cells[:, 0], offsets[:, 0])
    ])

    place = jax.ShapeDtypeStruct((4, held), jnp.float32)
    moments = jax.ShapeDtypeStruct((2, held), jnp.float32)
    piece = jax.ShapeDtypeStruct((2, own_count), jnp.float32)
    back = pltpu.VMEM((2, extent, extent), jnp.bfloat16)

    def deposited(guest, own):
        return pl.pallas_call(
            deposit_kernel,
            out_shape=(jax.ShapeDtypeStruct((extent, extent), jnp.float32), weight, weight, weight),
            in_specs=[VMEM] * 2,
            out_specs=(VMEM,) * 4,
            compiler_params=pltpu.CompilerParams(vmem_limit_bytes=WEIGHTS_VMEM),
            cost_estimate=pl.CostEstimate(
                flops=period**3 // 4, bytes_accessed=4 * period**2, transcendentals=0
            ),
            name="deposit",
        )(guest, own)

    def section(kernel, name, outs, arguments):
        return pl.pallas_call(
            kernel,
            out_shape=outs,
            in_specs=[VMEM] * (len(arguments) + 4),
            out_specs=(VMEM,) * len(outs),
            scratch_shapes=[back],
            compiler_params=pltpu.CompilerParams(vmem_limit_bytes=SECTION_VMEM),
            cost_estimate=pl.CostEstimate(
                flops=3 * period**3, bytes_accessed=8 * period**2, transcendentals=0
            ),
            name=name,
        )(*arguments, *tables)

    own, moment = section(
        first_kernel, "first", (place, moments),
        (cells[:, 0], offsets[:, 0], charges, momenta, other, even, slope, split),
    )
    for number in range(1, SECTIONS):
        guests = [exchange(own, 2 * number, further) for further in reversed(range(copies))]
        grid, *weights = deposited(guests.pop(0), own)
        guests.insert(0, grid)
        if number + 1 < SECTIONS:
            own, moment = section(
                functools.partial(middle_kernel, copies), "middle", (place, moments),
                (*guests, own, moment, *weights),
            )
        else:
            mine, theirs = section(
                functools.partial(last_kernel, copies), "last", (piece, piece),
                (*guests, moment, *weights),
            )
    received = exchange(theirs, 0)
    _, _, role = places_along(lax.axis_index("tr"))
    first = jnp.where(role == 1, mine, received)
    second = jnp.where(role == 1, received, mine)
    return jnp.stack([first, second])[:, None]


def solution(mesh):
    return jax.shard_map(
        per_device,
        mesh=mesh,
        in_specs=(
            P(None, "cuts", None, None),
            P(None, "cuts", None, None),
            P(None, "cuts", None),
            P(None, "cuts", None, "tr"),
            P(),
        ),
        out_specs=P(None, "cuts", None, "tr"),
        check_vma=False,
    )
```

```python
import functools
import math

import jax
import jax.numpy as jnp
import numpy as np
from jax import lax
from jax.experimental import pallas as pl
from jax.experimental.pallas import tpu as pltpu
from jax.sharding import PartitionSpec as P

SECTIONS = 4
DRIFT_STEP = 0.5
GROUP = 16
SETUP_VMEM = 32 * 1024 * 1024
WEIGHTS_VMEM = 16 * 1024 * 1024
SECTION_VMEM = 28 * 1024 * 1024
HALF_ROOT = math.sqrt(0.5)

VMEM = pl.BlockSpec(memory_space=pltpu.VMEM)
HBM = pl.BlockSpec(memory_space=pltpu.MemorySpace.HBM)


def dot_nn(left, right):
    return jnp.dot(left, right, preferred_element_type=jnp.float32)


def dot_nt(left, right):
    return lax.dot_general(
        left, right, (((1,), (1,)), ((), ())), preferred_element_type=jnp.float32
    )


def phases(products, period):
    theta = 2.0 * np.pi / period * (products % period)
    return np.cos(theta).astype(np.float32), np.sin(theta).astype(np.float32)


def factors(extent):
    half = extent // 2
    eighth = extent // 4
    period = 2 * extent
    cells = np.arange(extent, dtype=np.int64)
    split = np.concatenate([cells[0::2], cells[1::2]])
    odd = 2 * cells[:half] + 1
    fine = np.arange(GROUP, dtype=np.int64)
    coarse = np.arange(half // GROUP, dtype=np.int64)
    few = np.arange(eighth // GROUP, dtype=np.int64)
    starts = (8 * fine[None, :] + np.arange(8)[:, None]).reshape(-1)
    pieces = []
    pieces += phases(2 * GROUP * coarse[:, None] * split[None, :], 2 * period)
    pieces += phases((2 * fine + 1)[:, None] * split[None, :], 2 * period)
    for rows in (2 * GROUP * coarse, 2 * fine, 2 * fine + 1):
        pieces.append(np.concatenate(phases(rows[:, None] * odd[None, :], 2 * period), axis=1))
    for rows in (8 * GROUP * few, starts):
        both = np.concatenate(phases(rows[:, None] * cells[None, :eighth], period), axis=1)
        pieces.append(np.concatenate([both, both], axis=1))
    begins = np.cumsum([0] + [piece.shape[0] for piece in pieces])
    total = -(-int(begins[-1]) // 8) * 8
    packed = np.zeros((total, extent), np.float32)
    packed[: begins[-1]] = np.concatenate(pieces, axis=0)
    return packed, [int(begin) for begin in begins[:-1]]


def turned(cos_a, sin_a, cos_b, sin_b):
    return cos_a * cos_b - sin_a * sin_b, sin_a * cos_b + cos_a * sin_b


def added(left, right):
    return left[0] + right[0], left[1] + right[1]


def less(left, right):
    return left[0] - right[0], left[1] - right[1]


def times_i(value):
    return -value[1], value[0]


def four_points(values, turn):
    even, even_less = added(values[0], values[2]), less(values[0], values[2])
    odd, odd_less = added(values[1], values[3]), less(values[1], values[3])
    side = times_i(odd_less)
    up, down = added(even_less, side), less(even_less, side)
    if turn < 0:
        up, down = down, up
    return added(even, odd), up, less(even, odd), down


def eighths(values, turn):
    first, second, third, fourth = values
    plus = ((second[0] - turn * second[1]) * HALF_ROOT, (second[1] + turn * second[0]) * HALF_ROOT)
    third = times_i(third)
    if turn < 0:
        third = (-third[0], -third[1])
    minus = (
        (-fourth[0] - turn * fourth[1]) * HALF_ROOT,
        (turn * fourth[0] - fourth[1]) * HALF_ROOT,
    )
    return first, plus, third, minus


def joined(pair):
    return jnp.concatenate([pair[0].astype(jnp.bfloat16), pair[1].astype(jnp.bfloat16)], axis=1)


def spread(values):
    even = four_points(values, -1)
    odd = four_points(eighths(values, -1), -1)
    return [pair for couple in zip(even, odd) for pair in couple]


def gathered(values):
    even = four_points(values[0::2], 1)
    odd = eighths(four_points(values[1::2], 1), 1)
    return [added(left, right) for left, right in zip(even, odd)]


def places_along(shard):
    copy, side = shard // 2, shard % 2
    return copy, side, (side + copy) % 2


def my_place():
    shard = lax.axis_index("tr")
    copy = lax.div(shard, 2)
    side = lax.rem(shard, 2)
    return copy, side, lax.rem(side + copy, 2)


def setup_kernel(begins, green_ref, factor_ref, cells_ref, offsets_ref,
                 col_ref, inv_ref, row_ref, spec_ref, even_ref, slope_ref, split_ref,
                 green_vm, factor_vm, cells_vm, offsets_vm, sem):
    extent = col_ref.shape[1]
    half = extent // 2
    eighth = extent // 4
    period = 2 * extent
    small = [
        pltpu.make_async_copy(source, target, sem.at[8 + number])
        for number, (source, target) in enumerate(
            [(cells_ref, cells_vm), (offsets_ref, offsets_vm), (factor_ref, factor_vm)]
        )
    ]
    for copy in small:
        copy.start()
    copies = [
        pltpu.make_async_copy(
            green_ref.at[:, pl.ds(b * eighth, eighth)], green_vm.at[b], sem.at[b]
        )
        for b in range(8)
    ]
    for copy in copies:
        copy.start()
    copy_index, _, role = my_place()
    own = 1 - role
    small[0].wait()
    small[1].wait()
    width = even_ref.shape[1]
    lanes = pl.ds(pl.multiple_of(copy_index * width, width), width)
    place = cells_vm[own, :, lanes].astype(jnp.float32) + offsets_vm[own, :, lanes]
    store_weights(place, even_ref, slope_ref, split_ref)
    small[2].wait()

    for i in range(half // GROUP):
        rows = i * GROUP
        cosine, sine = turned(
            factor_vm[begins[0] + i : begins[0] + i + 1, :],
            factor_vm[begins[1] + i : begins[1] + i + 1, :],
            factor_vm[begins[2] : begins[2] + GROUP, :],
            factor_vm[begins[3] : begins[3] + GROUP, :],
        )
        col_ref[rows : rows + GROUP, :] = cosine.astype(jnp.bfloat16)
        col_ref[half + rows : half + rows + GROUP, :] = (-sine).astype(jnp.bfloat16)
        coarse = factor_vm[begins[4] + i : begins[4] + i + 1, :]
        for turn in range(2):
            fine = factor_vm[begins[5 + turn] : begins[5 + turn] + GROUP, :]
            cosine, sine = turned(coarse[:, :half], coarse[:, half:], fine[:, :half], fine[:, half:])
            at = turn * half + rows
            inv_ref[at : at + GROUP, :half] = cosine.astype(jnp.bfloat16)
            inv_ref[at : at + GROUP, half:] = (-sine).astype(jnp.bfloat16)
    for j in range(8):
        fine = factor_vm[begins[8] + j * GROUP : begins[8] + (j + 1) * GROUP, :]
        for i in range(eighth // GROUP):
            coarse = factor_vm[begins[7] + i : begins[7] + i + 1, :]
            cosine, sine = turned(
                coarse[:, :eighth], coarse[:, eighth:half], fine[:, :eighth], fine[:, eighth:half]
            )
            upper = i * GROUP
            lower = eighth + i * GROUP
            row_ref[j, upper : upper + GROUP, :eighth] = cosine.astype(jnp.bfloat16)
            row_ref[j, upper : upper + GROUP, eighth:] = sine.astype(jnp.bfloat16)
            row_ref[j, lower : lower + GROUP, :eighth] = (-sine).astype(jnp.bfloat16)
            row_ref[j, lower : lower + GROUP, eighth:] = cosine.astype(jnp.bfloat16)

    scale = 1.0 / (period * period)
    parity = lax.broadcasted_iota(jnp.int32, (half, eighth), 0) % 2
    sign = jnp.where(parity == 0, 1.0, -1.0)
    parts = [[], []]
    for b in range(4):
        copies[2 * b].wait()
        copies[2 * b + 1].wait()
        blocks = [
            joined([green_vm[2 * b + q, pl.ds(begin, half, stride=2), :] for q in range(2)])
            for begin in (0, 1, extent, extent + 1)
        ]
        for turn in range(2):
            table = frequency_rows(col_ref, turn)
            near = both_halves(table, blocks[0], blocks[1])
            far = both_halves(table, blocks[2], blocks[3])
            for q in range(2):
                cut = slice(q * eighth, (q + 1) * eighth)
                parts[turn].append(
                    (
                        (near[0][:, cut] - sign * far[1][:, cut]).astype(jnp.bfloat16),
                        (near[1][:, cut] + sign * far[0][:, cut]).astype(jnp.bfloat16),
                    )
                )
    for turn in range(2):
        part = parts[turn]
        even = four_points([added(part[q], part[q + 4]) for q in range(4)], -1)
        odd = four_points(eighths([less(part[q], part[q + 4]) for q in range(4)], -1), -1)
        sums = [pair for couple in zip(even, odd) for pair in couple]
        for j in range(8):
            spec = dot_nt(joined(sums[j]), row_ref[j]) * scale
            spec_ref[j, turn * half : (turn + 1) * half, :] = spec.astype(jnp.bfloat16)


def frequency_rows(col_ref, turn):
    half = col_ref.shape[0] // 2
    eighth = half // 2
    at = turn * eighth
    return jnp.concatenate(
        [col_ref[at : at + eighth, :], col_ref[half + at : half + at + eighth, :]], axis=0
    )


def both_halves(table, even_rows, odd_rows):
    half = table.shape[1] // 2
    eighth = half // 2
    even = dot_nn(table[:, :half], even_rows)
    odd = dot_nn(table[:, half:], odd_rows)
    plus, minus = even + odd, even - odd
    return (
        jnp.concatenate([plus[:eighth], minus[:eighth]], axis=0),
        jnp.concatenate([plus[eighth:], minus[eighth:]], axis=0),
    )


def codes(cells, half):
    return jnp.where(cells < half, cells, half - 1.0 - cells)


def chosen(extent, split, pairs):
    half = extent // 2
    width = pairs[0][0].shape[1]

    def raised(row):
        return jnp.broadcast_to(row, (GROUP, width)).astype(jnp.bfloat16)

    cells = [raised(codes(cell, half)) for cell, _ in pairs]
    weights = [raised(weight) for _, weight in pairs]
    count = lax.broadcasted_iota(jnp.int32, (GROUP, width), 0)
    blocks = []
    for begin in range(0, extent, GROUP):
        if split:
            nodes = 2 * (begin % half) + begin // half + 2 * count
        else:
            nodes = begin + count
        here = codes(nodes.astype(jnp.float32), half).astype(jnp.bfloat16)
        result = jnp.zeros_like(here)
        for cell, weight in zip(reversed(cells), reversed(weights)):
            result = jnp.where(here == cell, weight, result)
        blocks.append(result)
    return jnp.concatenate(blocks, axis=0)


def parted(position):
    cell = jnp.floor(position)
    return cell, position - cell


def hats(extent, split, position, weight=1.0):
    cell, part = parted(position)
    return chosen(extent, split, [(cell, weight * (1.0 - part)), (cell + 1.0, weight * part)])


def slopes(extent, position):
    cell, part = parted(position)
    return chosen(
        extent,
        False,
        [(cell - 1.0, 1.0 - part), (cell, part), (cell + 1.0, part - 1.0), (cell + 2.0, -part)],
    )


def store_weights(place, even_ref, slope_ref, split_ref):
    extent = even_ref.shape[0]
    even_ref[...] = hats(extent, False, place[1:2])
    slope_ref[...] = slopes(extent, place[1:2])
    split_ref[...] = hats(extent, True, place[0:1])


def deposit(place, charge, extent):
    weights_second = hats(extent, False, place[1:2])
    weights_first = hats(extent, True, place[0:1], charge)
    return dot_nt(weights_first, weights_second)


def deposit_kernel(guest_ref, own_ref, grid_ref, even_ref, slope_ref, split_ref):
    grid_ref[...] = deposit(guest_ref[0:2, :], guest_ref[2:3, :], grid_ref.shape[0])
    store_weights(own_ref[0:2, :], even_ref, slope_ref, split_ref)


def kicks(grid, even_ref, slope_ref, split_ref, col_ref, inv_ref, row_ref, spec_ref, back_ref):
    extent = col_ref.shape[1]
    half = extent // 2
    eighth = extent // 4
    grid = grid.astype(jnp.bfloat16)
    spreads = []
    for turn in range(2):
        real, imag = both_halves(frequency_rows(col_ref, turn), grid[:half], grid[half:])
        real, imag = real.astype(jnp.bfloat16), imag.astype(jnp.bfloat16)
        blocks = [
            (real[:, q * eighth : (q + 1) * eighth], imag[:, q * eighth : (q + 1) * eighth])
            for q in range(4)
        ]
        spreads.append(spread(blocks))
    for turn in range(2):
        here = slice(turn * half, (turn + 1) * half)
        backs = []
        for j, pair in enumerate(spreads[turn]):
            forward = dot_nt(joined(pair), row_ref[j]).astype(jnp.bfloat16)
            kernel_re = spec_ref[j, here, :eighth]
            kernel_im = spec_ref[j, here, eighth:]
            forward_re, forward_im = forward[:, :eighth], forward[:, eighth:]
            scaled = joined(
                (
                    forward_re * kernel_re - forward_im * kernel_im,
                    forward_re * kernel_im + forward_im * kernel_re,
                )
            )
            back = dot_nn(scaled, row_ref[j]).astype(jnp.bfloat16)
            backs.append((back[:, :eighth], back[:, eighth:]))
        for q, pair in enumerate(gathered(backs)):
            lanes = slice(q * eighth, (q + 1) * eighth)
            for part, value in enumerate(pair):
                where = slice(part * half + turn * eighth, part * half + (turn + 1) * eighth)
                low, high = value[:eighth], value[eighth:]
                back_ref[0, where, lanes] = low + high
                back_ref[1, where, lanes] = low - high
    even = dot_nn(inv_ref[:half, :], back_ref[0])
    odd = dot_nn(inv_ref[half:, :], back_ref[1])
    zero_row = jnp.zeros((1, extent), jnp.float32)
    before = jnp.concatenate([zero_row, odd[:-1]], axis=0)
    after = jnp.concatenate([even[1:], zero_row], axis=0)
    field = jnp.concatenate([before - odd, even - after], axis=0).astype(jnp.bfloat16)
    potential = jnp.concatenate([even, odd], axis=0).astype(jnp.bfloat16)

    def sampled(values, weights_ref):
        terms = dot_nn(values, weights_ref[...]).astype(jnp.bfloat16) * split_ref[...]
        count = extent
        while count > 16:
            count //= 2
            terms = terms[:count] + terms[count:]
        return jnp.sum(terms.astype(jnp.float32), axis=0, keepdims=True)

    return sampled(field, even_ref), sampled(potential, slope_ref)


def advance(position, moment, extent):
    return jnp.clip(position + DRIFT_STEP * moment, 1.0, extent - 2.0 - 1.0 / 64.0)


def store_moved(out_ref, moment_out_ref, place, charge, kick, moment, extent):
    for dim in range(2):
        line = slice(dim, dim + 1)
        total = moment[line] + kick[dim]
        moment_out_ref[line, :] = total
        out_ref[line, :] = advance(place[line], total, extent)
    out_ref[2:3, :] = charge
    out_ref[3:4, :] = charge


def first_kernel(cells_ref, offsets_ref, charges_ref, momenta_ref, other_ref, *rest):
    common = rest[:7]
    out_ref, moment_out_ref, back_ref = rest[7:]
    extent, width = common[0].shape
    copy_index, side, role = my_place()
    own, guest = 1 - role, role
    mine, other = momenta_ref[own], other_ref[own]
    moment = jnp.where(
        side == 0, jnp.concatenate([mine, other], axis=1), jnp.concatenate([other, mine], axis=1)
    )
    lanes = pl.ds(pl.multiple_of(copy_index * width, width), width)
    own_place = cells_ref[own, :, lanes].astype(jnp.float32) + offsets_ref[own, :, lanes]
    guest_place = cells_ref[guest].astype(jnp.float32) + offsets_ref[guest]
    grid = deposit(guest_place, charges_ref[guest], extent)
    kick = kicks(grid, *common, back_ref)
    charge = charges_ref[own, :, lanes]
    store_moved(out_ref, moment_out_ref, own_place, charge, kick, moment, extent)


def whole_grid(grid_ref, guest_refs):
    guest = jnp.concatenate([piece[...] for piece in guest_refs], axis=1)
    return grid_ref[...] + deposit(guest[0:2], guest[2:3], grid_ref.shape[0])


def middle_kernel(copies, *refs):
    grid = whole_grid(refs[0], refs[1:copies])
    own_ref, moment_ref = refs[copies : copies + 2]
    common = refs[copies + 2 : copies + 9]
    out_ref, moment_out_ref, back_ref = refs[copies + 9 :]
    kick = kicks(grid, *common, back_ref)
    own, extent = own_ref[...], common[0].shape[0]
    store_moved(out_ref, moment_out_ref, own[0:2], own[2:3], kick, moment_ref[...], extent)


def last_kernel(copies, *refs):
    grid = whole_grid(refs[0], refs[1:copies])
    moment_ref = refs[copies]
    common = refs[copies + 1 : copies + 8]
    mine_ref, theirs_ref, back_ref = refs[copies + 8 :]
    count = mine_ref.shape[1]
    kick = kicks(grid, *common, back_ref)
    total = jnp.concatenate([moment_ref[dim : dim + 1, :] + kick[dim] for dim in range(2)], axis=0)
    low, high = total[:, :count], total[:, count:]
    _, side, _ = my_place()
    mine_ref[...] = jnp.where(side == 0, low, high)
    theirs_ref[...] = jnp.where(side == 0, high, low)


def per_device(cells, offsets, charges, momenta, green):
    shards = lax.axis_size("tr")
    slices = lax.axis_size("cuts")
    period = green.shape[0]
    extent = period // 2
    particles = cells.shape[-1]
    own_count = momenta.shape[-1]

    def slot(cut, part):
        return (cut % slices) * shards + part

    copies = shards // 2

    def exchange(value, steps, further=0):
        pairs = []
        for cut in range(slices):
            for part in range(shards):
                copy, _, role = places_along(part)
                turn = steps if role == 1 else -steps
                goal = (copy + further) % copies
                side = (1 - role + goal) % 2
                pairs.append((slot(cut, part), slot(cut + turn, 2 * goal + side)))
        return lax.ppermute(value, ("cuts", "tr"), pairs)

    momenta = momenta[:, 0]
    other = exchange(momenta, 0)
    packed, begins = factors(extent)
    held = 2 * own_count
    weight = jax.ShapeDtypeStruct((extent, held), jnp.bfloat16)
    *tables, even, slope, split = pl.pallas_call(
        functools.partial(setup_kernel, begins),
        out_shape=(
            jax.ShapeDtypeStruct((extent, extent), jnp.bfloat16),
            jax.ShapeDtypeStruct((extent, extent), jnp.bfloat16),
            jax.ShapeDtypeStruct((8, extent // 2, extent // 2), jnp.bfloat16),
            jax.ShapeDtypeStruct((8, extent, extent // 2), jnp.bfloat16),
            weight, weight, weight,
        ),
        in_specs=[HBM] * 4,
        out_specs=(VMEM,) * 7,
        scratch_shapes=[
            pltpu.VMEM((8, period, extent // 4), jnp.float32),
            pltpu.VMEM(packed.shape, jnp.float32),
            pltpu.VMEM((2, 2, particles), jnp.int32),
            pltpu.VMEM((2, 2, particles), jnp.float32),
            pltpu.SemaphoreType.DMA((11,)),
        ],
        compiler_params=pltpu.CompilerParams(vmem_limit_bytes=SETUP_VMEM),
        cost_estimate=pl.CostEstimate(
            flops=2 * period**3, bytes_accessed=8 * period**2, transcendentals=0
        ),
        name="setup",
    )(*[
        pltpu.with_memory_space_constraint(value, pltpu.MemorySpace.HBM)
        for value in (green, jnp.asarray(packed), cells[:, 0], offsets[:, 0])
    ])

    place = jax.ShapeDtypeStruct((4, held), jnp.float32)
    moments = jax.ShapeDtypeStruct((2, held), jnp.float32)
    piece = jax.ShapeDtypeStruct((2, own_count), jnp.float32)
    back = pltpu.VMEM((2, extent, extent), jnp.bfloat16)

    def deposited(guest, own):
        return pl.pallas_call(
            deposit_kernel,
            out_shape=(jax.ShapeDtypeStruct((extent, extent), jnp.float32), weight, weight, weight),
            in_specs=[VMEM] * 2,
            out_specs=(VMEM,) * 4,
            compiler_params=pltpu.CompilerParams(vmem_limit_bytes=WEIGHTS_VMEM),
            cost_estimate=pl.CostEstimate(
                flops=period**3 // 4, bytes_accessed=4 * period**2, transcendentals=0
            ),
            name="deposit",
        )(guest, own)

    def section(kernel, name, outs, arguments):
        return pl.pallas_call(
            kernel,
            out_shape=outs,
            in_specs=[VMEM] * (len(arguments) + 4),
            out_specs=(VMEM,) * len(outs),
            scratch_shapes=[back],
            compiler_params=pltpu.CompilerParams(vmem_limit_bytes=SECTION_VMEM),
            cost_estimate=pl.CostEstimate(
                flops=3 * period**3, bytes_accessed=8 * period**2, transcendentals=0
            ),
            name=name,
        )(*arguments, *tables)

    own, moment = section(
        first_kernel, "first", (place, moments),
        (cells[:, 0], offsets[:, 0], charges, momenta, other, even, slope, split),
    )
    for number in range(1, SECTIONS):
        guests = [exchange(own, 2 * number, further) for further in reversed(range(copies))]
        grid, *weights = deposited(guests.pop(0), own)
        guests.insert(0, grid)
        if number + 1 < SECTIONS:
            own, moment = section(
                functools.partial(middle_kernel, copies), "middle", (place, moments),
                (*guests, own, moment, *weights),
            )
        else:
            mine, theirs = section(
                functools.partial(last_kernel, copies), "last", (piece, piece),
                (*guests, moment, *weights),
            )
    received = exchange(theirs, 0)
    _, _, role = places_along(lax.axis_index("tr"))
    first = jnp.where(role == 1, mine, received)
    second = jnp.where(role == 1, received, mine)
    return jnp.stack([first, second])[:, None]


def solution(mesh):
    return jax.shard_map(
        per_device,
        mesh=mesh,
        in_specs=(
            P(None, "cuts", None, None),
            P(None, "cuts", None, None),
            P(None, "cuts", None),
            P(None, "cuts", None, "tr"),
            P(),
        ),
        out_specs=P(None, "cuts", None, "tr"),
        check_vma=False,
    )
```

```python
import functools
import math

import jax
import jax.numpy as jnp
import numpy as np
from jax import lax
from jax.experimental import pallas as pl
from jax.experimental.pallas import tpu as pltpu
from jax.sharding import PartitionSpec as P

SECTIONS = 4
DRIFT_STEP = 0.5
GROUP = 16
SETUP_VMEM = 32 * 1024 * 1024
WEIGHTS_VMEM = 16 * 1024 * 1024
SECTION_VMEM = 28 * 1024 * 1024
HALF_ROOT = math.sqrt(0.5)

VMEM = pl.BlockSpec(memory_space=pltpu.VMEM)
HBM = pl.BlockSpec(memory_space=pltpu.MemorySpace.HBM)


def dot_nn(left, right):
    return jnp.dot(left, right, preferred_element_type=jnp.float32)


def dot_nt(left, right):
    return lax.dot_general(
        left, right, (((1,), (1,)), ((), ())), preferred_element_type=jnp.float32
    )


def phases(products, period):
    theta = 2.0 * np.pi / period * (products % period)
    return np.cos(theta).astype(np.float32), np.sin(theta).astype(np.float32)


def factors(extent):
    half = extent // 2
    eighth = extent // 4
    period = 2 * extent
    cells = np.arange(extent, dtype=np.int64)
    split = np.concatenate([cells[0::2], cells[1::2]])
    odd = 2 * cells[:half] + 1
    fine = np.arange(GROUP, dtype=np.int64)
    coarse = np.arange(half // GROUP, dtype=np.int64)
    few = np.arange(eighth // GROUP, dtype=np.int64)
    starts = (8 * fine[None, :] + np.arange(8)[:, None]).reshape(-1)
    pieces = []
    pieces += phases(2 * GROUP * coarse[:, None] * split[None, :], 2 * period)
    pieces += phases((2 * fine + 1)[:, None] * split[None, :], 2 * period)
    for rows in (2 * GROUP * coarse, 2 * fine, 2 * fine + 1):
        pieces.append(np.concatenate(phases(rows[:, None] * odd[None, :], 2 * period), axis=1))
    for rows in (8 * GROUP * few, starts):
        both = np.concatenate(phases(rows[:, None] * cells[None, :eighth], period), axis=1)
        pieces.append(np.concatenate([both, both], axis=1))
    begins = np.cumsum([0] + [piece.shape[0] for piece in pieces])
    total = -(-int(begins[-1]) // 8) * 8
    packed = np.zeros((total, extent), np.float32)
    packed[: begins[-1]] = np.concatenate(pieces, axis=0)
    return packed, [int(begin) for begin in begins[:-1]]


def turned(cos_a, sin_a, cos_b, sin_b):
    return cos_a * cos_b - sin_a * sin_b, sin_a * cos_b + cos_a * sin_b


def added(left, right):
    return left[0] + right[0], left[1] + right[1]


def less(left, right):
    return left[0] - right[0], left[1] - right[1]


def times_i(value):
    return -value[1], value[0]


def four_points(values, turn):
    even, even_less = added(values[0], values[2]), less(values[0], values[2])
    odd, odd_less = added(values[1], values[3]), less(values[1], values[3])
    side = times_i(odd_less)
    up, down = added(even_less, side), less(even_less, side)
    if turn < 0:
        up, down = down, up
    return added(even, odd), up, less(even, odd), down


def eighths(values, turn):
    first, second, third, fourth = values
    plus = ((second[0] - turn * second[1]) * HALF_ROOT, (second[1] + turn * second[0]) * HALF_ROOT)
    third = times_i(third)
    if turn < 0:
        third = (-third[0], -third[1])
    minus = (
        (-fourth[0] - turn * fourth[1]) * HALF_ROOT,
        (turn * fourth[0] - fourth[1]) * HALF_ROOT,
    )
    return first, plus, third, minus


def joined(pair):
    return jnp.concatenate([pair[0].astype(jnp.bfloat16), pair[1].astype(jnp.bfloat16)], axis=1)


def spread(values):
    even = four_points(values, -1)
    odd = four_points(eighths(values, -1), -1)
    return [pair for couple in zip(even, odd) for pair in couple]


def gathered(values):
    even = four_points(values[0::2], 1)
    odd = eighths(four_points(values[1::2], 1), 1)
    return [added(left, right) for left, right in zip(even, odd)]


def places_along(shard):
    copy, side = shard // 2, shard % 2
    return copy, side, (side + copy) % 2


def my_place():
    shard = lax.axis_index("tr")
    copy = lax.div(shard, 2)
    side = lax.rem(shard, 2)
    return copy, side, lax.rem(side + copy, 2)


def setup_kernel(begins, green_ref, factor_ref, cells_ref, offsets_ref,
                 col_ref, inv_ref, row_ref, spec_ref, even_ref, slope_ref, split_ref,
                 green_vm, factor_vm, cells_vm, offsets_vm, sem):
    extent = col_ref.shape[1]
    half = extent // 2
    eighth = extent // 4
    period = 2 * extent
    small = [
        pltpu.make_async_copy(source, target, sem.at[8 + number])
        for number, (source, target) in enumerate(
            [(cells_ref, cells_vm), (offsets_ref, offsets_vm), (factor_ref, factor_vm)]
        )
    ]
    for copy in small:
        copy.start()
    copies = [
        pltpu.make_async_copy(
            green_ref.at[:, pl.ds(b * eighth, eighth)], green_vm.at[b], sem.at[b]
        )
        for b in range(8)
    ]
    for copy in copies:
        copy.start()
    copy_index, _, role = my_place()
    own = 1 - role
    small[0].wait()
    small[1].wait()
    width = even_ref.shape[1]
    lanes = pl.ds(pl.multiple_of(copy_index * width, width), width)
    place = cells_vm[own, :, lanes].astype(jnp.float32) + offsets_vm[own, :, lanes]
    store_weights(place, even_ref, slope_ref, split_ref)
    small[2].wait()

    for i in range(half // GROUP):
        rows = i * GROUP
        cosine, sine = turned(
            factor_vm[begins[0] + i : begins[0] + i + 1, :],
            factor_vm[begins[1] + i : begins[1] + i + 1, :],
            factor_vm[begins[2] : begins[2] + GROUP, :],
            factor_vm[begins[3] : begins[3] + GROUP, :],
        )
        col_ref[rows : rows + GROUP, :] = cosine.astype(jnp.bfloat16)
        col_ref[half + rows : half + rows + GROUP, :] = (-sine).astype(jnp.bfloat16)
        coarse = factor_vm[begins[4] + i : begins[4] + i + 1, :]
        for turn in range(2):
            fine = factor_vm[begins[5 + turn] : begins[5 + turn] + GROUP, :]
            cosine, sine = turned(coarse[:, :half], coarse[:, half:], fine[:, :half], fine[:, half:])
            at = turn * half + rows
            inv_ref[at : at + GROUP, :half] = cosine.astype(jnp.bfloat16)
            inv_ref[at : at + GROUP, half:] = (-sine).astype(jnp.bfloat16)
    for j in range(8):
        fine = factor_vm[begins[8] + j * GROUP : begins[8] + (j + 1) * GROUP, :]
        for i in range(eighth // GROUP):
            coarse = factor_vm[begins[7] + i : begins[7] + i + 1, :]
            cosine, sine = turned(
                coarse[:, :eighth], coarse[:, eighth:half], fine[:, :eighth], fine[:, eighth:half]
            )
            upper = i * GROUP
            lower = eighth + i * GROUP
            row_ref[j, upper : upper + GROUP, :eighth] = cosine.astype(jnp.bfloat16)
            row_ref[j, upper : upper + GROUP, eighth:] = sine.astype(jnp.bfloat16)
            row_ref[j, lower : lower + GROUP, :eighth] = (-sine).astype(jnp.bfloat16)
            row_ref[j, lower : lower + GROUP, eighth:] = cosine.astype(jnp.bfloat16)

    scale = 1.0 / (period * period)
    parity = lax.broadcasted_iota(jnp.int32, (half, eighth), 0) % 2
    sign = jnp.where(parity == 0, 1.0, -1.0)
    parts = [[], []]
    for b in range(4):
        copies[2 * b].wait()
        copies[2 * b + 1].wait()
        blocks = [
            joined([green_vm[2 * b + q, pl.ds(begin, half, stride=2), :] for q in range(2)])
            for begin in (0, 1, extent, extent + 1)
        ]
        for turn in range(2):
            table = frequency_rows(col_ref, turn)
            near = both_halves(table, blocks[0], blocks[1])
            far = both_halves(table, blocks[2], blocks[3])
            for q in range(2):
                cut = slice(q * eighth, (q + 1) * eighth)
                parts[turn].append(
                    (
                        (near[0][:, cut] - sign * far[1][:, cut]).astype(jnp.bfloat16),
                        (near[1][:, cut] + sign * far[0][:, cut]).astype(jnp.bfloat16),
                    )
                )
    for turn in range(2):
        part = parts[turn]
        even = four_points([added(part[q], part[q + 4]) for q in range(4)], -1)
        odd = four_points(eighths([less(part[q], part[q + 4]) for q in range(4)], -1), -1)
        sums = [pair for couple in zip(even, odd) for pair in couple]
        for j in range(8):
            spec = dot_nt(joined(sums[j]), row_ref[j]) * scale
            spec_ref[j, turn * half : (turn + 1) * half, :] = spec.astype(jnp.bfloat16)


def frequency_rows(col_ref, turn):
    half = col_ref.shape[0] // 2
    eighth = half // 2
    at = turn * eighth
    return jnp.concatenate(
        [col_ref[at : at + eighth, :], col_ref[half + at : half + at + eighth, :]], axis=0
    )


def both_halves(table, even_rows, odd_rows):
    half = table.shape[1] // 2
    eighth = half // 2
    even = dot_nn(table[:, :half], even_rows)
    odd = dot_nn(table[:, half:], odd_rows)
    plus, minus = even + odd, even - odd
    return (
        jnp.concatenate([plus[:eighth], minus[:eighth]], axis=0),
        jnp.concatenate([plus[eighth:], minus[eighth:]], axis=0),
    )


def codes(cells, half):
    return jnp.where(cells < half, cells, half - 1.0 - cells)


def chosen(extent, split, pairs):
    half = extent // 2
    width = pairs[0][0].shape[1]

    def raised(row):
        return jnp.broadcast_to(row, (GROUP, width)).astype(jnp.bfloat16)

    cells = [raised(codes(cell, half)) for cell, _ in pairs]
    weights = [raised(weight) for _, weight in pairs]
    count = lax.broadcasted_iota(jnp.int32, (GROUP, width), 0)
    blocks = []
    for begin in range(0, extent, GROUP):
        if split:
            nodes = 2 * (begin % half) + begin // half + 2 * count
        else:
            nodes = begin + count
        here = codes(nodes.astype(jnp.float32), half).astype(jnp.bfloat16)
        result = jnp.zeros_like(here)
        for cell, weight in zip(reversed(cells), reversed(weights)):
            result = jnp.where(here == cell, weight, result)
        blocks.append(result)
    return jnp.concatenate(blocks, axis=0)


def parted(position):
    cell = jnp.floor(position)
    return cell, position - cell


def hats(extent, split, position, weight=1.0):
    cell, part = parted(position)
    return chosen(extent, split, [(cell, weight * (1.0 - part)), (cell + 1.0, weight * part)])


def slopes(extent, position):
    cell, part = parted(position)
    return chosen(
        extent,
        False,
        [(cell - 1.0, 1.0 - part), (cell, part), (cell + 1.0, part - 1.0), (cell + 2.0, -part)],
    )


def store_weights(place, even_ref, slope_ref, split_ref):
    extent = even_ref.shape[0]
    even_ref[...] = hats(extent, False, place[1:2])
    slope_ref[...] = slopes(extent, place[1:2])
    split_ref[...] = hats(extent, True, place[0:1])


def deposit(place, charge, extent):
    weights_second = hats(extent, False, place[1:2])
    weights_first = hats(extent, True, place[0:1], charge)
    return dot_nt(weights_first, weights_second)


def deposit_kernel(guest_ref, own_ref, grid_ref, even_ref, slope_ref, split_ref):
    grid_ref[...] = deposit(guest_ref[0:2, :], guest_ref[2:3, :], grid_ref.shape[0])
    store_weights(own_ref[0:2, :], even_ref, slope_ref, split_ref)


def kicks(grid, even_ref, slope_ref, split_ref, col_ref, inv_ref, row_ref, spec_ref, back_ref):
    extent = col_ref.shape[1]
    half = extent // 2
    eighth = extent // 4
    grid = grid.astype(jnp.bfloat16)
    halves = [
        both_halves(frequency_rows(col_ref, turn), grid[:half], grid[half:]) for turn in range(2)
    ]
    real, imag = (
        jnp.concatenate([pair[part] for pair in halves], axis=0).astype(jnp.bfloat16)
        for part in range(2)
    )
    blocks = [
        (real[:, q * eighth : (q + 1) * eighth], imag[:, q * eighth : (q + 1) * eighth])
        for q in range(4)
    ]
    backs = []
    for j, pair in enumerate(spread(blocks)):
        forward = dot_nt(joined(pair), row_ref[j]).astype(jnp.bfloat16)
        kernel_re = spec_ref[j, :, :eighth]
        kernel_im = spec_ref[j, :, eighth:]
        forward_re, forward_im = forward[:, :eighth], forward[:, eighth:]
        scaled = joined(
            (
                forward_re * kernel_re - forward_im * kernel_im,
                forward_re * kernel_im + forward_im * kernel_re,
            )
        )
        back = dot_nn(scaled, row_ref[j]).astype(jnp.bfloat16)
        backs.append((back[:, :eighth], back[:, eighth:]))
    for q, pair in enumerate(gathered(backs)):
        lanes = slice(q * eighth, (q + 1) * eighth)
        for part, value in enumerate(pair):
            for turn in range(2):
                where = slice(part * half + turn * eighth, part * half + (turn + 1) * eighth)
                low = value[turn * half : turn * half + eighth]
                high = value[turn * half + eighth : (turn + 1) * half]
                back_ref[0, where, lanes] = low + high
                back_ref[1, where, lanes] = low - high
    even = dot_nn(inv_ref[:half, :], back_ref[0])
    odd = dot_nn(inv_ref[half:, :], back_ref[1])
    zero_row = jnp.zeros((1, extent), jnp.float32)
    before = jnp.concatenate([zero_row, odd[:-1]], axis=0)
    after = jnp.concatenate([even[1:], zero_row], axis=0)
    field = jnp.concatenate([before - odd, even - after], axis=0).astype(jnp.bfloat16)
    potential = jnp.concatenate([even, odd], axis=0).astype(jnp.bfloat16)

    def sampled(values, weights_ref):
        terms = dot_nn(values, weights_ref[...]).astype(jnp.bfloat16) * split_ref[...]
        count = extent
        while count > 16:
            count //= 2
            terms = terms[:count] + terms[count:]
        return jnp.sum(terms.astype(jnp.float32), axis=0, keepdims=True)

    return sampled(field, even_ref), sampled(potential, slope_ref)


def advance(position, moment, extent):
    return jnp.clip(position + DRIFT_STEP * moment, 1.0, extent - 2.0 - 1.0 / 64.0)


def store_moved(out_ref, moment_out_ref, place, charge, kick, moment, extent):
    for dim in range(2):
        line = slice(dim, dim + 1)
        total = moment[line] + kick[dim]
        moment_out_ref[line, :] = total
        out_ref[line, :] = advance(place[line], total, extent)
    out_ref[2:3, :] = charge
    out_ref[3:4, :] = charge


def first_kernel(cells_ref, offsets_ref, charges_ref, momenta_ref, other_ref, *rest):
    common = rest[:7]
    out_ref, moment_out_ref, back_ref = rest[7:]
    extent, width = common[0].shape
    copy_index, side, role = my_place()
    own, guest = 1 - role, role
    mine, other = momenta_ref[own], other_ref[own]
    moment = jnp.where(
        side == 0, jnp.concatenate([mine, other], axis=1), jnp.concatenate([other, mine], axis=1)
    )
    lanes = pl.ds(pl.multiple_of(copy_index * width, width), width)
    own_place = cells_ref[own, :, lanes].astype(jnp.float32) + offsets_ref[own, :, lanes]
    guest_place = cells_ref[guest].astype(jnp.float32) + offsets_ref[guest]
    grid = deposit(guest_place, charges_ref[guest], extent)
    kick = kicks(grid, *common, back_ref)
    charge = charges_ref[own, :, lanes]
    store_moved(out_ref, moment_out_ref, own_place, charge, kick, moment, extent)


def whole_grid(grid_ref, guest_refs):
    guest = jnp.concatenate([piece[...] for piece in guest_refs], axis=1)
    return grid_ref[...] + deposit(guest[0:2], guest[2:3], grid_ref.shape[0])


def middle_kernel(copies, *refs):
    grid = whole_grid(refs[0], refs[1:copies])
    own_ref, moment_ref = refs[copies : copies + 2]
    common = refs[copies + 2 : copies + 9]
    out_ref, moment_out_ref, back_ref = refs[copies + 9 :]
    kick = kicks(grid, *common, back_ref)
    own, extent = own_ref[...], common[0].shape[0]
    store_moved(out_ref, moment_out_ref, own[0:2], own[2:3], kick, moment_ref[...], extent)


def last_kernel(copies, *refs):
    grid = whole_grid(refs[0], refs[1:copies])
    moment_ref = refs[copies]
    common = refs[copies + 1 : copies + 8]
    mine_ref, theirs_ref, back_ref = refs[copies + 8 :]
    count = mine_ref.shape[1]
    kick = kicks(grid, *common, back_ref)
    total = jnp.concatenate([moment_ref[dim : dim + 1, :] + kick[dim] for dim in range(2)], axis=0)
    low, high = total[:, :count], total[:, count:]
    _, side, _ = my_place()
    mine_ref[...] = jnp.where(side == 0, low, high)
    theirs_ref[...] = jnp.where(side == 0, high, low)


def per_device(cells, offsets, charges, momenta, green):
    shards = lax.axis_size("tr")
    slices = lax.axis_size("cuts")
    period = green.shape[0]
    extent = period // 2
    particles = cells.shape[-1]
    own_count = momenta.shape[-1]

    def slot(cut, part):
        return (cut % slices) * shards + part

    copies = shards // 2

    def exchange(value, steps, further=0):
        pairs = []
        for cut in range(slices):
            for part in range(shards):
                copy, _, role = places_along(part)
                turn = steps if role == 1 else -steps
                goal = (copy + further) % copies
                side = (1 - role + goal) % 2
                pairs.append((slot(cut, part), slot(cut + turn, 2 * goal + side)))
        return lax.ppermute(value, ("cuts", "tr"), pairs)

    momenta = momenta[:, 0]
    other = exchange(momenta, 0)
    packed, begins = factors(extent)
    held = 2 * own_count
    weight = jax.ShapeDtypeStruct((extent, held), jnp.bfloat16)
    *tables, even, slope, split = pl.pallas_call(
        functools.partial(setup_kernel, begins),
        out_shape=(
            jax.ShapeDtypeStruct((extent, extent), jnp.bfloat16),
            jax.ShapeDtypeStruct((extent, extent), jnp.bfloat16),
            jax.ShapeDtypeStruct((8, extent // 2, extent // 2), jnp.bfloat16),
            jax.ShapeDtypeStruct((8, extent, extent // 2), jnp.bfloat16),
            weight, weight, weight,
        ),
        in_specs=[HBM] * 4,
        out_specs=(VMEM,) * 7,
        scratch_shapes=[
            pltpu.VMEM((8, period, extent // 4), jnp.float32),
            pltpu.VMEM(packed.shape, jnp.float32),
            pltpu.VMEM((2, 2, particles), jnp.int32),
            pltpu.VMEM((2, 2, particles), jnp.float32),
            pltpu.SemaphoreType.DMA((11,)),
        ],
        compiler_params=pltpu.CompilerParams(vmem_limit_bytes=SETUP_VMEM),
        cost_estimate=pl.CostEstimate(
            flops=2 * period**3, bytes_accessed=8 * period**2, transcendentals=0
        ),
        name="setup",
    )(*[
        pltpu.with_memory_space_constraint(value, pltpu.MemorySpace.HBM)
        for value in (green, jnp.asarray(packed), cells[:, 0], offsets[:, 0])
    ])

    place = jax.ShapeDtypeStruct((4, held), jnp.float32)
    moments = jax.ShapeDtypeStruct((2, held), jnp.float32)
    piece = jax.ShapeDtypeStruct((2, own_count), jnp.float32)
    back = pltpu.VMEM((2, extent, extent), jnp.bfloat16)

    def deposited(guest, own):
        return pl.pallas_call(
            deposit_kernel,
            out_shape=(jax.ShapeDtypeStruct((extent, extent), jnp.float32), weight, weight, weight),
            in_specs=[VMEM] * 2,
            out_specs=(VMEM,) * 4,
            compiler_params=pltpu.CompilerParams(vmem_limit_bytes=WEIGHTS_VMEM),
            cost_estimate=pl.CostEstimate(
                flops=period**3 // 4, bytes_accessed=4 * period**2, transcendentals=0
            ),
            name="deposit",
        )(guest, own)

    def section(kernel, name, outs, arguments):
        return pl.pallas_call(
            kernel,
            out_shape=outs,
            in_specs=[VMEM] * (len(arguments) + 4),
            out_specs=(VMEM,) * len(outs),
            scratch_shapes=[back],
            compiler_params=pltpu.CompilerParams(vmem_limit_bytes=SECTION_VMEM),
            cost_estimate=pl.CostEstimate(
                flops=3 * period**3, bytes_accessed=8 * period**2, transcendentals=0
            ),
            name=name,
        )(*arguments, *tables)

    own, moment = section(
        first_kernel, "first", (place, moments),
        (cells[:, 0], offsets[:, 0], charges, momenta, other, even, slope, split),
    )
    for number in range(1, SECTIONS):
        guests = [exchange(own, 2 * number, further) for further in reversed(range(copies))]
        grid, *weights = deposited(guests.pop(0), own)
        guests.insert(0, grid)
        if number + 1 < SECTIONS:
            own, moment = section(
                functools.partial(middle_kernel, copies), "middle", (place, moments),
                (*guests, own, moment, *weights),
            )
        else:
            mine, theirs = section(
                functools.partial(last_kernel, copies), "last", (piece, piece),
                (*guests, moment, *weights),
            )
    received = exchange(theirs, 0)
    _, _, role = places_along(lax.axis_index("tr"))
    first = jnp.where(role == 1, mine, received)
    second = jnp.where(role == 1, received, mine)
    return jnp.stack([first, second])[:, None]


def solution(mesh):
    return jax.shard_map(
        per_device,
        mesh=mesh,
        in_specs=(
            P(None, "cuts", None, None),
            P(None, "cuts", None, None),
            P(None, "cuts", None),
            P(None, "cuts", None, "tr"),
            P(),
        ),
        out_specs=P(None, "cuts", None, "tr"),
        check_vma=False,
    )
```

```python
import functools
import math

import jax
import jax.numpy as jnp
import numpy as np
from jax import lax
from jax.experimental import pallas as pl
from jax.experimental.pallas import tpu as pltpu
from jax.sharding import PartitionSpec as P

SECTIONS = 4
DRIFT_STEP = 0.5
GROUP = 16
SETUP_VMEM = 32 * 1024 * 1024
WEIGHTS_VMEM = 16 * 1024 * 1024
SECTION_VMEM = 28 * 1024 * 1024
HALF_ROOT = math.sqrt(0.5)

VMEM = pl.BlockSpec(memory_space=pltpu.VMEM)
HBM = pl.BlockSpec(memory_space=pltpu.MemorySpace.HBM)


def dot_nn(left, right):
    return jnp.dot(left, right, preferred_element_type=jnp.float32)


def dot_nt(left, right):
    return lax.dot_general(
        left, right, (((1,), (1,)), ((), ())), preferred_element_type=jnp.float32
    )


def phases(products, period):
    theta = 2.0 * np.pi / period * (products % period)
    return np.cos(theta).astype(np.float32), np.sin(theta).astype(np.float32)


def factors(extent):
    half = extent // 2
    eighth = extent // 4
    period = 2 * extent
    cells = np.arange(extent, dtype=np.int64)
    split = np.concatenate([cells[0::2], cells[1::2]])
    odd = 2 * cells[:half] + 1
    fine = np.arange(GROUP, dtype=np.int64)
    coarse = np.arange(half // GROUP, dtype=np.int64)
    few = np.arange(eighth // GROUP, dtype=np.int64)
    starts = (8 * fine[None, :] + np.arange(8)[:, None]).reshape(-1)
    pieces = []
    pieces += phases(2 * GROUP * coarse[:, None] * split[None, :], 2 * period)
    pieces += phases((2 * fine + 1)[:, None] * split[None, :], 2 * period)
    for rows in (2 * GROUP * coarse, 2 * fine, 2 * fine + 1):
        pieces.append(np.concatenate(phases(rows[:, None] * odd[None, :], 2 * period), axis=1))
    for rows in (8 * GROUP * few, starts):
        both = np.concatenate(phases(rows[:, None] * cells[None, :eighth], period), axis=1)
        pieces.append(np.concatenate([both, both], axis=1))
    begins = np.cumsum([0] + [piece.shape[0] for piece in pieces])
    total = -(-int(begins[-1]) // 8) * 8
    packed = np.zeros((total, extent), np.float32)
    packed[: begins[-1]] = np.concatenate(pieces, axis=0)
    return packed, [int(begin) for begin in begins[:-1]]


def turned(cos_a, sin_a, cos_b, sin_b):
    return cos_a * cos_b - sin_a * sin_b, sin_a * cos_b + cos_a * sin_b


def added(left, right):
    return left[0] + right[0], left[1] + right[1]


def less(left, right):
    return left[0] - right[0], left[1] - right[1]


def times_i(value):
    return -value[1], value[0]


def four_points(values, turn):
    even, even_less = added(values[0], values[2]), less(values[0], values[2])
    odd, odd_less = added(values[1], values[3]), less(values[1], values[3])
    side = times_i(odd_less)
    up, down = added(even_less, side), less(even_less, side)
    if turn < 0:
        up, down = down, up
    return added(even, odd), up, less(even, odd), down


def eighths(values, turn):
    first, second, third, fourth = values
    plus = ((second[0] - turn * second[1]) * HALF_ROOT, (second[1] + turn * second[0]) * HALF_ROOT)
    third = times_i(third)
    if turn < 0:
        third = (-third[0], -third[1])
    minus = (
        (-fourth[0] - turn * fourth[1]) * HALF_ROOT,
        (turn * fourth[0] - fourth[1]) * HALF_ROOT,
    )
    return first, plus, third, minus


def joined(pair):
    return jnp.concatenate([pair[0].astype(jnp.bfloat16), pair[1].astype(jnp.bfloat16)], axis=1)


def spread(values):
    even = four_points(values, -1)
    odd = four_points(eighths(values, -1), -1)
    return [pair for couple in zip(even, odd) for pair in couple]


def gathered(values):
    even = four_points(values[0::2], 1)
    odd = eighths(four_points(values[1::2], 1), 1)
    return [added(left, right) for left, right in zip(even, odd)]


def places_along(shard):
    copy, side = shard // 2, shard % 2
    return copy, side, (side + copy) % 2


def my_place():
    shard = lax.axis_index("tr")
    copy = lax.div(shard, 2)
    side = lax.rem(shard, 2)
    return copy, side, lax.rem(side + copy, 2)


def setup_kernel(begins, green_ref, factor_ref, cells_ref, offsets_ref,
                 col_ref, inv_ref, row_ref, spec_ref, even_ref, slope_ref, split_ref,
                 green_vm, factor_vm, cells_vm, offsets_vm, sem):
    extent = col_ref.shape[1]
    half = extent // 2
    eighth = extent // 4
    period = 2 * extent
    small = [
        pltpu.make_async_copy(source, target, sem.at[8 + number])
        for number, (source, target) in enumerate(
            [(cells_ref, cells_vm), (offsets_ref, offsets_vm), (factor_ref, factor_vm)]
        )
    ]
    for copy in small:
        copy.start()
    copies = [
        pltpu.make_async_copy(
            green_ref.at[:, pl.ds(b * eighth, eighth)], green_vm.at[b], sem.at[b]
        )
        for b in range(8)
    ]
    for copy in copies:
        copy.start()
    copy_index, _, role = my_place()
    own = 1 - role
    small[0].wait()
    small[1].wait()
    width = even_ref.shape[1]
    lanes = pl.ds(pl.multiple_of(copy_index * width, width), width)
    place = cells_vm[own, :, lanes].astype(jnp.float32) + offsets_vm[own, :, lanes]
    store_weights(place, even_ref, slope_ref, split_ref)
    small[2].wait()

    for i in range(half // GROUP):
        rows = i * GROUP
        cosine, sine = turned(
            factor_vm[begins[0] + i : begins[0] + i + 1, :],
            factor_vm[begins[1] + i : begins[1] + i + 1, :],
            factor_vm[begins[2] : begins[2] + GROUP, :],
            factor_vm[begins[3] : begins[3] + GROUP, :],
        )
        col_ref[rows : rows + GROUP, :] = cosine.astype(jnp.bfloat16)
        col_ref[half + rows : half + rows + GROUP, :] = (-sine).astype(jnp.bfloat16)
        coarse = factor_vm[begins[4] + i : begins[4] + i + 1, :]
        for turn in range(2):
            fine = factor_vm[begins[5 + turn] : begins[5 + turn] + GROUP, :]
            cosine, sine = turned(coarse[:, :half], coarse[:, half:], fine[:, :half], fine[:, half:])
            at = turn * half + rows
            inv_ref[at : at + GROUP, :half] = cosine.astype(jnp.bfloat16)
            inv_ref[at : at + GROUP, half:] = (-sine).astype(jnp.bfloat16)
    for j in range(8):
        fine = factor_vm[begins[8] + j * GROUP : begins[8] + (j + 1) * GROUP, :]
        for i in range(eighth // GROUP):
            coarse = factor_vm[begins[7] + i : begins[7] + i + 1, :]
            cosine, sine = turned(
                coarse[:, :eighth], coarse[:, eighth:half], fine[:, :eighth], fine[:, eighth:half]
            )
            upper = i * GROUP
            lower = eighth + i * GROUP
            row_ref[j, upper : upper + GROUP, :eighth] = cosine.astype(jnp.bfloat16)
            row_ref[j, upper : upper + GROUP, eighth:] = sine.astype(jnp.bfloat16)
            row_ref[j, lower : lower + GROUP, :eighth] = (-sine).astype(jnp.bfloat16)
            row_ref[j, lower : lower + GROUP, eighth:] = cosine.astype(jnp.bfloat16)

    scale = 1.0 / (period * period)
    parity = lax.broadcasted_iota(jnp.int32, (extent, eighth), 0) % 2
    sign = jnp.where(parity == 0, 1.0, -1.0)
    parts = []
    for b in range(4):
        copies[2 * b].wait()
        copies[2 * b + 1].wait()
        blocks = [
            joined([green_vm[2 * b + q, pl.ds(begin, half, stride=2), :] for q in range(2)])
            for begin in (0, 1, extent, extent + 1)
        ]
        near = both_halves(col_ref, blocks[0], blocks[1])
        far = both_halves(col_ref, blocks[2], blocks[3])
        for q in range(2):
            cut = slice(q * eighth, (q + 1) * eighth)
            parts.append(
                (
                    (near[0][:, cut] - sign * far[1][:, cut]).astype(jnp.bfloat16),
                    (near[1][:, cut] + sign * far[0][:, cut]).astype(jnp.bfloat16),
                )
            )
    even = four_points([added(parts[q], parts[q + 4]) for q in range(4)], -1)
    odd = four_points(eighths([less(parts[q], parts[q + 4]) for q in range(4)], -1), -1)
    sums = [pair for couple in zip(even, odd) for pair in couple]
    for j in range(8):
        spec_ref[j] = (dot_nt(joined(sums[j]), row_ref[j]) * scale).astype(jnp.bfloat16)


def both_halves(col_ref, even_rows, odd_rows):
    half = col_ref.shape[0] // 2
    eighth = half // 2
    even = dot_nn(col_ref[:, :half], even_rows)
    odd = dot_nn(col_ref[:, half:], odd_rows)
    plus, minus = even + odd, even - odd

    def ordered(begin):
        pieces = []
        for at in (begin, begin + eighth):
            pieces += [plus[at : at + eighth], minus[at : at + eighth]]
        return jnp.concatenate(pieces, axis=0)

    return ordered(0), ordered(half)


def codes(cells, half):
    return jnp.where(cells < half, cells, half - 1.0 - cells)


def chosen(extent, split, pairs):
    half = extent // 2
    width = pairs[0][0].shape[1]

    def raised(row):
        return jnp.broadcast_to(row, (GROUP, width)).astype(jnp.bfloat16)

    cells = [raised(codes(cell, half)) for cell, _ in pairs]
    weights = [raised(weight) for _, weight in pairs]
    count = lax.broadcasted_iota(jnp.int32, (GROUP, width), 0)
    blocks = []
    for begin in range(0, extent, GROUP):
        if split:
            nodes = 2 * (begin % half) + begin // half + 2 * count
        else:
            nodes = begin + count
        here = codes(nodes.astype(jnp.float32), half).astype(jnp.bfloat16)
        result = jnp.zeros_like(here)
        for cell, weight in zip(reversed(cells), reversed(weights)):
            result = jnp.where(here == cell, weight, result)
        blocks.append(result)
    return jnp.concatenate(blocks, axis=0)


def parted(position):
    cell = jnp.floor(position)
    return cell, position - cell


def hats(extent, split, position, weight=1.0):
    cell, part = parted(position)
    return chosen(extent, split, [(cell, weight * (1.0 - part)), (cell + 1.0, weight * part)])


def slopes(extent, position):
    cell, part = parted(position)
    return chosen(
        extent,
        False,
        [(cell - 1.0, 1.0 - part), (cell, part), (cell + 1.0, part - 1.0), (cell + 2.0, -part)],
    )


def store_weights(place, even_ref, slope_ref, split_ref):
    extent = even_ref.shape[0]
    even_ref[...] = hats(extent, False, place[1:2])
    slope_ref[...] = slopes(extent, place[1:2])
    split_ref[...] = hats(extent, True, place[0:1])


def deposit(place, charge, extent):
    weights_second = hats(extent, False, place[1:2])
    weights_first = hats(extent, True, place[0:1], charge)
    return dot_nt(weights_first, weights_second)


def deposit_kernel(guest_ref, own_ref, grid_ref, even_ref, slope_ref, split_ref):
    grid_ref[...] = deposit(guest_ref[0:2, :], guest_ref[2:3, :], grid_ref.shape[0])
    store_weights(own_ref[0:2, :], even_ref, slope_ref, split_ref)


def kicks(grid, even_ref, slope_ref, split_ref, col_ref, inv_ref, row_ref, spec_ref, back_ref):
    extent = col_ref.shape[1]
    half = extent // 2
    eighth = extent // 4
    grid = grid.astype(jnp.bfloat16)
    real, imag = (
        part.astype(jnp.bfloat16) for part in both_halves(col_ref, grid[:half], grid[half:])
    )
    blocks = [
        (real[:, q * eighth : (q + 1) * eighth], imag[:, q * eighth : (q + 1) * eighth])
        for q in range(4)
    ]
    backs = []
    for j, pair in enumerate(spread(blocks)):
        forward = dot_nt(joined(pair), row_ref[j]).astype(jnp.bfloat16)
        kernel_re = spec_ref[j, :, :eighth]
        kernel_im = spec_ref[j, :, eighth:]
        forward_re, forward_im = forward[:, :eighth], forward[:, eighth:]
        scaled = joined(
            (
                forward_re * kernel_re - forward_im * kernel_im,
                forward_re * kernel_im + forward_im * kernel_re,
            )
        )
        back = dot_nn(scaled, row_ref[j]).astype(jnp.bfloat16)
        backs.append((back[:, :eighth], back[:, eighth:]))
    for q, pair in enumerate(gathered(backs)):
        lanes = slice(q * eighth, (q + 1) * eighth)
        for part, value in enumerate(pair):
            for turn in range(2):
                where = slice(part * half + turn * eighth, part * half + (turn + 1) * eighth)
                low = value[turn * half : turn * half + eighth]
                high = value[turn * half + eighth : (turn + 1) * half]
                back_ref[0, where, lanes] = low + high
                back_ref[1, where, lanes] = low - high
    even = dot_nn(inv_ref[:half, :], back_ref[0])
    odd = dot_nn(inv_ref[half:, :], back_ref[1])
    zero_row = jnp.zeros((1, extent), jnp.float32)
    before = jnp.concatenate([zero_row, odd[:-1]], axis=0)
    after = jnp.concatenate([even[1:], zero_row], axis=0)
    field = jnp.concatenate([before - odd, even - after], axis=0).astype(jnp.bfloat16)
    potential = jnp.concatenate([even, odd], axis=0).astype(jnp.bfloat16)

    def sampled(values, weights_ref):
        terms = dot_nn(values, weights_ref[...]).astype(jnp.bfloat16) * split_ref[...]
        count = extent
        while count > 16:
            count //= 2
            terms = terms[:count] + terms[count:]
        return jnp.sum(terms.astype(jnp.float32), axis=0, keepdims=True)

    return sampled(field, even_ref), sampled(potential, slope_ref)


def advance(position, moment, extent):
    return jnp.clip(position + DRIFT_STEP * moment, 1.0, extent - 2.0 - 1.0 / 64.0)


def store_moved(out_ref, moment_out_ref, place, charge, kick, moment, extent):
    for dim in range(2):
        line = slice(dim, dim + 1)
        total = moment[line] + kick[dim]
        moment_out_ref[line, :] = total
        out_ref[line, :] = advance(place[line], total, extent)
    out_ref[2:3, :] = charge
    out_ref[3:4, :] = charge


def first_kernel(cells_ref, offsets_ref, charges_ref, momenta_ref, other_ref, *rest):
    common = rest[:7]
    out_ref, moment_out_ref, back_ref = rest[7:]
    extent, width = common[0].shape
    copy_index, side, role = my_place()
    own, guest = 1 - role, role
    mine, other = momenta_ref[own], other_ref[own]
    moment = jnp.where(
        side == 0, jnp.concatenate([mine, other], axis=1), jnp.concatenate([other, mine], axis=1)
    )
    lanes = pl.ds(pl.multiple_of(copy_index * width, width), width)
    own_place = cells_ref[own, :, lanes].astype(jnp.float32) + offsets_ref[own, :, lanes]
    guest_place = cells_ref[guest].astype(jnp.float32) + offsets_ref[guest]
    grid = deposit(guest_place, charges_ref[guest], extent)
    kick = kicks(grid, *common, back_ref)
    charge = charges_ref[own, :, lanes]
    store_moved(out_ref, moment_out_ref, own_place, charge, kick, moment, extent)


def whole_grid(grid_ref, guest_refs):
    guest = jnp.concatenate([piece[...] for piece in guest_refs], axis=1)
    return grid_ref[...] + deposit(guest[0:2], guest[2:3], grid_ref.shape[0])


def middle_kernel(copies, *refs):
    grid = whole_grid(refs[0], refs[1:copies])
    own_ref, moment_ref = refs[copies : copies + 2]
    common = refs[copies + 2 : copies + 9]
    out_ref, moment_out_ref, back_ref = refs[copies + 9 :]
    kick = kicks(grid, *common, back_ref)
    own, extent = own_ref[...], common[0].shape[0]
    store_moved(out_ref, moment_out_ref, own[0:2], own[2:3], kick, moment_ref[...], extent)


def last_kernel(copies, *refs):
    grid = whole_grid(refs[0], refs[1:copies])
    moment_ref = refs[copies]
    common = refs[copies + 1 : copies + 8]
    mine_ref, theirs_ref, back_ref = refs[copies + 8 :]
    count = mine_ref.shape[1]
    kick = kicks(grid, *common, back_ref)
    total = jnp.concatenate([moment_ref[dim : dim + 1, :] + kick[dim] for dim in range(2)], axis=0)
    low, high = total[:, :count], total[:, count:]
    _, side, _ = my_place()
    mine_ref[...] = jnp.where(side == 0, low, high)
    theirs_ref[...] = jnp.where(side == 0, high, low)


def per_device(cells, offsets, charges, momenta, green):
    shards = lax.axis_size("tr")
    slices = lax.axis_size("cuts")
    period = green.shape[0]
    extent = period // 2
    particles = cells.shape[-1]
    own_count = momenta.shape[-1]

    def slot(cut, part):
        return (cut % slices) * shards + part

    copies = shards // 2

    def exchange(value, steps, further=0):
        pairs = []
        for cut in range(slices):
            for part in range(shards):
                copy, _, role = places_along(part)
                turn = steps if role == 1 else -steps
                goal = (copy + further) % copies
                side = (1 - role + goal) % 2
                pairs.append((slot(cut, part), slot(cut + turn, 2 * goal + side)))
        return lax.ppermute(value, ("cuts", "tr"), pairs)

    momenta = momenta[:, 0]
    other = exchange(momenta, 0)
    packed, begins = factors(extent)
    held = 2 * own_count
    weight = jax.ShapeDtypeStruct((extent, held), jnp.bfloat16)
    *tables, even, slope, split = pl.pallas_call(
        functools.partial(setup_kernel, begins),
        out_shape=(
            jax.ShapeDtypeStruct((extent, extent), jnp.bfloat16),
            jax.ShapeDtypeStruct((extent, extent), jnp.bfloat16),
            jax.ShapeDtypeStruct((8, extent // 2, extent // 2), jnp.bfloat16),
            jax.ShapeDtypeStruct((8, extent, extent // 2), jnp.bfloat16),
            weight, weight, weight,
        ),
        in_specs=[HBM] * 4,
        out_specs=(VMEM,) * 7,
        scratch_shapes=[
            pltpu.VMEM((8, period, extent // 4), jnp.float32),
            pltpu.VMEM(packed.shape, jnp.float32),
            pltpu.VMEM((2, 2, particles), jnp.int32),
            pltpu.VMEM((2, 2, particles), jnp.float32),
            pltpu.SemaphoreType.DMA((11,)),
        ],
        compiler_params=pltpu.CompilerParams(vmem_limit_bytes=SETUP_VMEM),
        cost_estimate=pl.CostEstimate(
            flops=2 * period**3, bytes_accessed=8 * period**2, transcendentals=0
        ),
        name="setup",
    )(*[
        pltpu.with_memory_space_constraint(value, pltpu.MemorySpace.HBM)
        for value in (green, jnp.asarray(packed), cells[:, 0], offsets[:, 0])
    ])

    place = jax.ShapeDtypeStruct((4, held), jnp.float32)
    moments = jax.ShapeDtypeStruct((2, held), jnp.float32)
    piece = jax.ShapeDtypeStruct((2, own_count), jnp.float32)
    back = pltpu.VMEM((2, extent, extent), jnp.bfloat16)

    def deposited(guest, own):
        return pl.pallas_call(
            deposit_kernel,
            out_shape=(jax.ShapeDtypeStruct((extent, extent), jnp.float32), weight, weight, weight),
            in_specs=[VMEM] * 2,
            out_specs=(VMEM,) * 4,
            compiler_params=pltpu.CompilerParams(vmem_limit_bytes=WEIGHTS_VMEM),
            cost_estimate=pl.CostEstimate(
                flops=period**3 // 4, bytes_accessed=4 * period**2, transcendentals=0
            ),
            name="deposit",
        )(guest, own)

    def section(kernel, name, outs, arguments):
        return pl.pallas_call(
            kernel,
            out_shape=outs,
            in_specs=[VMEM] * (len(arguments) + 4),
            out_specs=(VMEM,) * len(outs),
            scratch_shapes=[back],
            compiler_params=pltpu.CompilerParams(vmem_limit_bytes=SECTION_VMEM),
            cost_estimate=pl.CostEstimate(
                flops=3 * period**3, bytes_accessed=8 * period**2, transcendentals=0
            ),
            name=name,
        )(*arguments, *tables)

    own, moment = section(
        first_kernel, "first", (place, moments),
        (cells[:, 0], offsets[:, 0], charges, momenta, other, even, slope, split),
    )
    for number in range(1, SECTIONS):
        guests = [exchange(own, 2 * number, further) for further in reversed(range(copies))]
        grid, *weights = deposited(guests.pop(0), own)
        guests.insert(0, grid)
        if number + 1 < SECTIONS:
            own, moment = section(
                functools.partial(middle_kernel, copies), "middle", (place, moments),
                (*guests, own, moment, *weights),
            )
        else:
            mine, theirs = section(
                functools.partial(last_kernel, copies), "last", (piece, piece),
                (*guests, moment, *weights),
            )
    received = exchange(theirs, 0)
    _, _, role = places_along(lax.axis_index("tr"))
    first = jnp.where(role == 1, mine, received)
    second = jnp.where(role == 1, received, mine)
    return jnp.stack([first, second])[:, None]


def solution(mesh):
    return jax.shard_map(
        per_device,
        mesh=mesh,
        in_specs=(
            P(None, "cuts", None, None),
            P(None, "cuts", None, None),
            P(None, "cuts", None),
            P(None, "cuts", None, "tr"),
            P(),
        ),
        out_specs=P(None, "cuts", None, "tr"),
        check_vma=False,
    )
```
